256 devices in a mesh: chain: 2 (over y), gz: 16 (over z), gy: 4 (over x), pa: 2 (over core).
Axes of the slice: x: 4, y: 2, z: 16, core: 2. Of those that a mesh axis runs over, the one named last changes fastest.
The devices are a block of a 4x16x16 slice.
Arguments:
- probes: float32 [32, 128, 128, 256], P(('chain', 'pa'), 'gz', 'gy'), parts along dimension 0, may hold values from -6 to 6
- velocity: float32 [3, 256, 128, 256], P(None, ('chain', 'gz'), 'gy'), parts along dimension 1, may hold values from -0.3 to 0.3
- prior_scale: float32 [256, 128, 256], P(('chain', 'gz'), 'gy'), parts along dimension 0, may hold values from 0.3 to 3
- noise_precision: float32 [256, 128, 256], P(('chain', 'gz'), 'gy'), parts along dimension 0, may hold values from 0.3 to 3
- source_mask: int32 [256, 128, 256], P(('chain', 'gz'), 'gy'), parts along dimension 0, may hold values 0 or 1
- sensor_mask: int32 [256, 128, 256], P(('chain', 'gz'), 'gy'), parts along dimension 0, may hold values 0 or 1
Outputs:
- hessian: float32 [32, 128, 128, 256], P(('chain', 'pa'), 'gz', 'gy'), parts along dimension 0
- gram: float32 [32, 16], P(('chain', 'pa')), parts along dimension 0
The draws below stay inside these ranges and needn't reach their ends.
There are 2 independent parts, one for each index of `chain`. The reference program is written for one: setup_inputs(seed, part) draws one part's arguments, and reference() takes and returns one part's arrays. A program takes and returns all parts, laid end to end along the dimension named above; each array names one. Nothing has to cross between parts.
All inputs are finite; a program needn't handle non-finite values. No bound on the sum of `source_mask` or of `sensor_mask` on one device may be relied on, other than what follows from the above.
Results may differ from the reference program's by a relative error of at most 0.0003.
Values sent between devices are 32-bit elements; how exact they have to be, the bound alone decides.
A program may use at most 128 MiB of HBM per device.

```python
import math
import jax
import jax.numpy as jnp
from jax import lax

NX = 256
P_SIZE = 16
STEPS = 5
NY = 128
NZ = 128


def touch_ends(values, rng, low, largest):
    longest = values.shape.index(max(values.shape))
    spots = []
    for shift in (0, 1):
        where = [jax.random.randint(jax.random.fold_in(rng, axis), (), 0, length) for axis, length in enumerate(values.shape)]
        where[longest] = (where[longest] + shift) % values.shape[longest]
        spots.append(tuple(where))
    return values.at[spots[0]].set(low).at[spots[1]].set(largest)


def block_scale(rng, extent, shards, low, high):
    level = 1.0
    for dim, parts in shards:
        heights = jax.random.uniform(jax.random.fold_in(jax.random.fold_in(rng, 6), dim), (parts,), jnp.float32, low / len(shards), high / len(shards))
        level = level * jnp.repeat(jnp.exp(heights), extent[dim] // parts).reshape((-1,) + (1,) * (len(extent) - 1 - dim))
    return level


def scatter_about(own_key, shape, deviation, bound, cuts=(), kind=jnp.bfloat16):
    drawn = deviation * jax.random.normal(own_key, shape, jnp.float32)
    if cuts:
        drawn = drawn * block_scale(own_key, shape, cuts, -0.22, 0.18)
    return jnp.clip(drawn, -bound, bound).astype(kind)


def setup_inputs(seed: int = 0, part: int = 0) -> dict:
    splits = jax.random.split(jax.random.key(seed), 7)
    own_keys = jax.random.split(jax.random.fold_in(splits[6], part), 7)
    probes = scatter_about(own_keys[0], (P_SIZE, NZ, NY, NX), 1.0, 6.0, ((0, 2), (1, 16), (2, 4)), jnp.float32)
    velocity = jnp.clip(jax.random.uniform(own_keys[1], (3, NZ, NY, NX), jnp.float32, -0.3, 0.3) * block_scale(own_keys[1], (3, NZ, NY, NX), ((1, 16), (2, 4)), -0.4, 0.0), -0.3, 0.3)
    prior_scale = jnp.clip(jnp.exp(math.log(3.0) - 2.3025851 * jax.random.uniform(own_keys[2], (NZ, NY, NX), jnp.float32) ** block_scale(own_keys[2], (NZ, NY, NX), ((0, 16), (1, 4)), -0.2, 0.2)), 0.3, 3.0)
    noise_precision = jnp.clip(jnp.exp(math.log(3.0) - 2.3025851 * jax.random.uniform(own_keys[3], (NZ, NY, NX), jnp.float32) ** block_scale(own_keys[3], (NZ, NY, NX), ((0, 16), (1, 4)), -0.2, 0.2)), 0.3, 3.0)
    source_mask = touch_ends((jax.random.randint(own_keys[4], (NZ, NY, NX), 0, 2) < 1).astype(jnp.int32), jax.random.fold_in(own_keys[4], 1), 0, 1)
    sensor_mask = touch_ends((jax.random.randint(own_keys[5], (NZ, NY, NX), 0, 4) < 1).astype(jnp.int32), jax.random.fold_in(own_keys[5], 1), 0, 1)
    return {"probes": probes, "velocity": velocity, "prior_scale": prior_scale, "noise_precision": noise_precision, "source_mask": source_mask, "sensor_mask": sensor_mask}


diffuse_cross = 0.15
diffuse_along = 16.0

def shift_cells(field, offset):
    zeros = jnp.zeros(field.shape[:-1] + (1,), jnp.float32)
    if offset > 0:
        return jnp.concatenate([field[..., 1:], zeros], -1)
    return jnp.concatenate([zeros, field[..., :-1]], -1)

def apply_implicit(field, matrix):
    flat = field.reshape(-1, field.shape[-1])
    return jnp.dot(flat.astype(jnp.float32), matrix.astype(jnp.float32), precision=lax.Precision.HIGHEST, preferred_element_type=jnp.float32).reshape(field.shape)

def forward_explicit(padded, coef_pad):
    centre = padded[:, 1:-1, 1:-1]
    plus_z = padded[:, 2:, 1:-1]
    minus_z = padded[:, :-2, 1:-1]
    plus_y = padded[:, 1:-1, 2:]
    minus_y = padded[:, 1:-1, :-2]
    speeds = coef_pad[:3, 1:-1, 1:-1]
    laplace = plus_z + minus_z + plus_y + minus_y - 4.0 * centre
    drift = speeds[0] * (shift_cells(centre, 1) - shift_cells(centre, -1))
    drift = drift + speeds[1] * (plus_y - minus_y) + speeds[2] * (plus_z - minus_z)
    return centre + diffuse_cross * laplace - 0.5 * drift

def adjoint_explicit(padded, coef_pad):
    centre = padded[:, 1:-1, 1:-1]
    laplace = padded[:, 2:, 1:-1] + padded[:, :-2, 1:-1] + padded[:, 1:-1, 2:] + padded[:, 1:-1, :-2] - 4.0 * centre
    flux_x = coef_pad[0, 1:-1, 1:-1] * centre
    flux_y = coef_pad[1, 1:-1, :] * padded[:, 1:-1, :]
    flux_z = coef_pad[2, :, 1:-1] * padded[:, :, 1:-1]
    drift = shift_cells(flux_x, 1) - shift_cells(flux_x, -1)
    drift = drift + flux_y[:, :, 2:] - flux_y[:, :, :-2] + flux_z[:, 2:] - flux_z[:, :-2]
    return centre + diffuse_cross * laplace + 0.5 * drift

def solve_probes(work, coef_pad, matrix, padder):
    weight_src = coef_pad[3, 1:-1, 1:-1]
    weight_obs = coef_pad[4, 1:-1, 1:-1]
    source = weight_src * work
    state = apply_implicit(source, matrix)
    states = [state]
    for counter in range(1, STEPS):
        state = apply_implicit(forward_explicit(padder(state), coef_pad) + source, matrix)
        states.append(state)
    adjoint = weight_obs * states[-1]
    pulled = apply_implicit(adjoint, matrix)
    gradient = pulled
    for counter in range(STEPS - 2, -1, -1):
        adjoint = weight_obs * states[counter] + adjoint_explicit(padder(pulled), coef_pad)
        pulled = apply_implicit(adjoint, matrix)
        gradient = gradient + pulled
    return weight_src * gradient

def pad_field(field):
    return jnp.pad(field, ((0, 0), (1, 1), (1, 1), (0, 0)))

def reference(probes, velocity, prior_scale, noise_precision, source_mask, sensor_mask):
    weight_src = source_mask.astype(jnp.float32) * prior_scale
    weight_obs = sensor_mask.astype(jnp.float32) * noise_precision
    coeffs = jnp.concatenate([velocity, weight_src[None], weight_obs[None]], 0)
    coef_pad = pad_field(coeffs)
    length = probes.shape[-1]
    eye = jnp.eye(length, dtype=jnp.float32)
    banded = (1.0 + 2.0 * diffuse_along) * eye - diffuse_along * (jnp.eye(length, k=1, dtype=jnp.float32) + jnp.eye(length, k=-1, dtype=jnp.float32))
    matrix = jnp.linalg.inv(banded)
    hessian = solve_probes(probes, coef_pad, matrix, pad_field)
    count = probes.shape[0]
    cells = probes.shape[1] * probes.shape[2] * probes.shape[3]
    gram = jnp.einsum('ac,bc->ab', probes.reshape(count, -1), hessian.reshape(count, -1), precision=lax.Precision.HIGHEST) / cells
    return (hessian, gram)
```

```python
import functools

import jax
import jax.numpy as jnp
import numpy as np
from jax import lax
from jax.experimental import pallas as pl
from jax.experimental.pallas import tpu as pltpu
from jax.sharding import PartitionSpec as P

MESH = pl.DeviceIdType.MESH
STEPS = 5
SUB = 8

diffuse_cross = 0.15
diffuse_along = 16.0

ZLO, ZHI, YLO, YHI = range(4)
CZP, CZM, CYP, CYM, CXP, CXM, SRC, OBS = range(8)


def implicit_matrix(length):
    banded = (1.0 + 2.0 * diffuse_along) * np.eye(length) - diffuse_along * (
        np.eye(length, k=1) + np.eye(length, k=-1)
    )
    matrix = np.linalg.inv(banded).astype(np.float32)
    high = matrix.astype(jnp.bfloat16)
    low = (matrix - high.astype(np.float32)).astype(jnp.bfloat16)
    return jnp.asarray(high), jnp.asarray(low)


def kernel(
    probes_ref,
    vel_ref,
    prior_ref,
    noise_ref,
    smask_ref,
    omask_ref,
    mhi_ref,
    mlo_ref,
    out_ref,
    u_ref,
    s_ref,
    b_ref,
    coef_ref,
    whi_ref,
    wlo_ref,
    zh_ref,
    yh_ref,
    zs_ref,
    ys_ref,
    send_sem,
    recv_sem,
):
    count, nz, ny, nx = probes_ref.shape
    tiles = ny // SUB
    zi, yi = lax.axis_index("gz"), lax.axis_index("gy")
    zn, yn = lax.axis_size("gz"), lax.axis_size("gy")
    exists = [zi > 0, zi < zn - 1, yi > 0, yi < yn - 1]
    target = [
        {"gz": lax.max(zi - 1, 0)},
        {"gz": lax.min(zi + 1, zn - 1)},
        {"gy": lax.max(yi - 1, 0)},
        {"gy": lax.min(yi + 1, yn - 1)},
    ]

    barrier = pltpu.get_barrier_semaphore()
    for side in range(4):

        @pl.when(exists[side])
        def _():
            pl.semaphore_signal(barrier, inc=1, device_id=target[side], device_id_type=MESH)

    row = lax.broadcasted_iota(jnp.int32, (SUB, nx), 0)
    first_row, last_row = row == 0, row == SUB - 1
    lane = lax.broadcasted_iota(jnp.int32, (ny, nx), 1)

    def prepare(z, _):
        vx, vy, vz = (0.5 * vel_ref[c, z] for c in range(3))
        coef_ref[CZP, z] = diffuse_cross - vz
        coef_ref[CZM, z] = diffuse_cross + vz
        coef_ref[CYP, z] = diffuse_cross - vy
        coef_ref[CYM, z] = diffuse_cross + vy
        coef_ref[CXP, z] = jnp.where(lane == nx - 1, 0.0, -vx)
        coef_ref[CXM, z] = jnp.where(lane == 0, 0.0, vx)
        coef_ref[SRC, z] = smask_ref[z].astype(jnp.float32) * prior_ref[z]
        coef_ref[OBS, z] = omask_ref[z].astype(jnp.float32) * noise_ref[z]
        return 0

    lax.fori_loop(0, nz, prepare, 0)

    @pl.when(zi == 0)
    def _():
        zh_ref[:, 0] = jnp.zeros(zh_ref.shape[:1] + zh_ref.shape[2:], jnp.float32)

    @pl.when(zi == zn - 1)
    def _():
        zh_ref[:, 1] = jnp.zeros(zh_ref.shape[:1] + zh_ref.shape[2:], jnp.float32)

    @pl.when(yi == 0)
    def _():
        yh_ref[:, 0] = jnp.zeros(yh_ref.shape[:1] + yh_ref.shape[2:], jnp.float32)

    @pl.when(yi == yn - 1)
    def _():
        yh_ref[:, 1] = jnp.zeros(yh_ref.shape[:1] + yh_ref.shape[2:], jnp.float32)

    pl.semaphore_wait(barrier, sum(side.astype(jnp.int32) for side in exists))

    def copies(slot, p, sources):
        result = []
        for side in range(4):
            halo = zh_ref if side < 2 else yh_ref
            result.append(
                pltpu.make_async_remote_copy(
                    src_ref=sources[side],
                    dst_ref=halo.at[slot, (side % 2) ^ 1, p],
                    send_sem=send_sem.at[slot, side, p],
                    recv_sem=recv_sem.at[slot, side ^ 1, p],
                    device_id=target[side],
                    device_id_type=MESH,
                )
            )
        return result

    def send(slot, p, sources):
        for side, copy in enumerate(copies(slot, p, sources)):
            pl.when(exists[side])(copy.start)

    def settle(slot, p, sources):
        moved = copies(slot, p, sources)
        for side in range(4):

            @pl.when(exists[side])
            def _():
                moved[side ^ 1].wait_recv()
                moved[side].wait_send()

    def state_sources(n, slot, p):
        return [u_ref.at[n, p, 0], u_ref.at[n, p, nz - 1], ys_ref.at[slot, 0, p], ys_ref.at[slot, 1, p]]

    def adjoint_sources(slot, p):
        return [zs_ref.at[slot, 0, p], zs_ref.at[slot, 1, p], ys_ref.at[slot, 0, p], ys_ref.at[slot, 1, p]]

    def put(z, pair, left, right):
        rows = jnp.concatenate([left, right], axis=0)
        high = rows.astype(jnp.bfloat16)
        low = (rows - high.astype(jnp.float32)).astype(jnp.bfloat16)
        where = pl.ds(z * ny + pair * 2 * SUB, 2 * SUB)
        whi_ref[where, :] = high
        wlo_ref[where, :] = low

    def solve():
        dot = functools.partial(jnp.dot, preferred_element_type=jnp.float32)
        high, low = whi_ref[...], wlo_ref[...]
        moved = dot(high, mhi_ref[...]) + (dot(high, mlo_ref[...]) + dot(low, mhi_ref[...]))
        return moved.reshape(nz, ny, nx)

    def by_tile(make):
        for z in range(nz):
            for pair in range(tiles // 2):
                put(z, pair, make(z, 2 * pair), make(z, 2 * pair + 1))

    def rows_of(t):
        return pl.ds(t * SUB, SUB)

    def coef(kind, z, t):
        return coef_ref[kind, z, rows_of(t), :]

    def forward(n, slot, p):
        def make(z, t):
            def at(zz, tt):
                return u_ref[n, p, zz, rows_of(tt), :]

            centre = at(z, t)
            plus_z = at(z + 1, t) if z < nz - 1 else zh_ref[slot, 1, p, rows_of(t), :]
            minus_z = at(z - 1, t) if z > 0 else zh_ref[slot, 0, p, rows_of(t), :]
            if t < tiles - 1:
                above = pltpu.roll(at(z, t + 1), SUB - 1, 0)
            else:
                above = jnp.broadcast_to(yh_ref[slot, 1, p, pl.ds(z, 1), :], (SUB, nx))
            if t > 0:
                below = pltpu.roll(at(z, t - 1), 1, 0)
            else:
                below = jnp.broadcast_to(yh_ref[slot, 0, p, pl.ds(z, 1), :], (SUB, nx))
            plus_y = jnp.where(last_row, above, pltpu.roll(centre, SUB - 1, 0))
            minus_y = jnp.where(first_row, below, pltpu.roll(centre, 1, 0))
            total = (1.0 - 4.0 * diffuse_cross) * centre + s_ref[p, z, rows_of(t), :]
            total = total + (coef(CZP, z, t) * plus_z + coef(CZM, z, t) * minus_z)
            total = total + (coef(CYP, z, t) * plus_y + coef(CYM, z, t) * minus_y)
            return total + (
                coef(CXP, z, t) * pltpu.roll(centre, nx - 1, 1) + coef(CXM, z, t) * pltpu.roll(centre, 1, 1)
            )

        by_tile(make)

    def backward(n, slot, p):
        def make(z, t):
            def at(zz, tt):
                return b_ref[p, zz, rows_of(tt), :]

            centre = at(z, t)
            if z < nz - 1:
                plus_z = coef(CZM, z + 1, t) * at(z + 1, t)
            else:
                plus_z = zh_ref[slot, 1, p, rows_of(t), :]
            if z > 0:
                minus_z = coef(CZP, z - 1, t) * at(z - 1, t)
            else:
                minus_z = zh_ref[slot, 0, p, rows_of(t), :]
            if t < tiles - 1:
                above = pltpu.roll(coef(CYM, z, t + 1) * at(z, t + 1), SUB - 1, 0)
            else:
                above = jnp.broadcast_to(yh_ref[slot, 1, p, pl.ds(z, 1), :], (SUB, nx))
            if t > 0:
                below = pltpu.roll(coef(CYP, z, t - 1) * at(z, t - 1), 1, 0)
            else:
                below = jnp.broadcast_to(yh_ref[slot, 0, p, pl.ds(z, 1), :], (SUB, nx))
            plus_y = jnp.where(last_row, above, pltpu.roll(coef(CYM, z, t) * centre, SUB - 1, 0))
            minus_y = jnp.where(first_row, below, pltpu.roll(coef(CYP, z, t) * centre, 1, 0))
            total = (1.0 - 4.0 * diffuse_cross) * centre + coef(OBS, z, t) * u_ref[n, p, z, rows_of(t), :]
            total = total + (plus_z + minus_z)
            total = total + (plus_y + minus_y)
            return total + (
                pltpu.roll(coef(CXM, z, t) * centre, nx - 1, 1) + pltpu.roll(coef(CXP, z, t) * centre, 1, 1)
            )

        by_tile(make)

    def finish_state(n, slot, p):
        state = solve()
        u_ref[n, p] = state
        for z in range(nz):
            ys_ref[slot, 0, p, pl.ds(z, 1), :] = state[z, 0:1, :]
            ys_ref[slot, 1, p, pl.ds(z, 1), :] = state[z, ny - 1 : ny, :]

    def finish_adjoint(slot, p, pulled):
        b_ref[p] = pulled
        zs_ref[slot, 0, p] = coef_ref[CZM, 0] * pulled[0]
        zs_ref[slot, 1, p] = coef_ref[CZP, nz - 1] * pulled[nz - 1]
        for z in range(nz):
            ys_ref[slot, 0, p, pl.ds(z, 1), :] = coef_ref[CYM, z, 0:1, :] * pulled[z, 0:1, :]
            ys_ref[slot, 1, p, pl.ds(z, 1), :] = coef_ref[CYP, z, ny - 1 : ny, :] * pulled[z, ny - 1 : ny, :]

    last = STEPS - 1

    def first_step(p, _):
        for z in range(nz):
            for t in range(tiles):
                s_ref[p, z, rows_of(t), :] = coef(SRC, z, t) * probes_ref[p, z, rows_of(t), :]
        by_tile(lambda z, t: coef(SRC, z, t) * probes_ref[p, z, rows_of(t), :])
        finish_state(0, 0, p)
        send(0, p, state_sources(0, 0, p))
        return 0

    lax.fori_loop(0, count, first_step, 0)

    def forward_step(i, _):
        n, p = i // count + 1, i % count
        before, now = (n + 1) % 2, n % 2
        settle(before, p, state_sources(n - 1, before, p))
        forward(n - 1, before, p)
        finish_state(n, now, p)
        send(now, p, state_sources(n, now, p))
        return 0

    lax.fori_loop(0, (last - 1) * count, forward_step, 0)

    def turn_step(p, _):
        before, now = (last + 1) % 2, last % 2
        settle(before, p, state_sources(last - 1, before, p))
        forward(last - 1, before, p)
        u_ref[last, p] = solve()
        by_tile(lambda z, t: coef(OBS, z, t) * u_ref[last, p, z, rows_of(t), :])
        pulled = solve()
        out_ref[p] = pulled
        finish_adjoint(now, p, pulled)
        send(now, p, adjoint_sources(now, p))
        return 0

    lax.fori_loop(0, count, turn_step, 0)

    def backward_step(i, _):
        k, p = i // count + 1, i % count
        before, now = (last + k + 1) % 2, (last + k) % 2
        settle(before, p, adjoint_sources(before, p))
        backward(last - k, before, p)
        pulled = solve()
        out_ref[p] += pulled
        finish_adjoint(now, p, pulled)
        send(now, p, adjoint_sources(now, p))
        return 0

    lax.fori_loop(0, (last - 1) * count, backward_step, 0)

    def last_step(p, _):
        before = (2 * last + 1) % 2
        settle(before, p, adjoint_sources(before, p))
        backward(0, before, p)
        out_ref[p] = coef_ref[SRC] * (out_ref[p] + solve())
        return 0

    lax.fori_loop(0, count, last_step, 0)


def by_axis(array, axes):
    return functools.reduce(lax.psum, axes, array)


def shards(probes, velocity, prior_scale, noise_precision, source_mask, sensor_mask):
    count, nz, ny, nx = probes.shape
    high, low = implicit_matrix(nx)
    vmem = pl.BlockSpec(memory_space=pltpu.VMEM)
    hessian = pl.pallas_call(
        kernel,
        out_shape=jax.ShapeDtypeStruct(probes.shape, jnp.float32),
        in_specs=[vmem] * 8,
        out_specs=vmem,
        scratch_shapes=[
            pltpu.VMEM((STEPS, count, nz, ny, nx), jnp.float32),
            pltpu.VMEM((count, nz, ny, nx), jnp.float32),
            pltpu.VMEM((count, nz, ny, nx), jnp.float32),
            pltpu.VMEM((8, nz, ny, nx), jnp.float32),
            pltpu.VMEM((nz * ny, nx), jnp.bfloat16),
            pltpu.VMEM((nz * ny, nx), jnp.bfloat16),
            pltpu.VMEM((2, 2, count, ny, nx), jnp.float32),
            pltpu.VMEM((2, 2, count, nz, nx), jnp.float32),
            pltpu.VMEM((2, 2, count, ny, nx), jnp.float32),
            pltpu.VMEM((2, 2, count, nz, nx), jnp.float32),
            pltpu.SemaphoreType.DMA((2, 4, count)),
            pltpu.SemaphoreType.DMA((2, 4, count)),
        ],
        compiler_params=pltpu.CompilerParams(
            collective_id=0, has_side_effects=True, vmem_limit_bytes=48 * 1024 * 1024
        ),
        name="solve",
    )(probes, velocity, prior_scale, noise_precision, source_mask, sensor_mask, high, low)
    own_rows = probes.reshape(count, -1)
    piece = lax.all_gather(hessian, "pa", axis=0, tiled=True)
    partial_gram = jnp.einsum(
        "ac,bc->ab", own_rows, piece.reshape(piece.shape[0], -1), precision=lax.Precision.HIGHEST
    )
    total_cells = nz * ny * nx * lax.axis_size("gz") * lax.axis_size("gy")
    gram = by_axis(partial_gram, ("gz", "gy")) / total_cells
    return (hessian, gram)


def solution(mesh):
    in_specs = (
        P(("chain", "pa"), "gz", "gy", None),
        P(None, ("chain", "gz"), "gy", None),
        P(("chain", "gz"), "gy", None),
        P(("chain", "gz"), "gy", None),
        P(("chain", "gz"), "gy", None),
        P(("chain", "gz"), "gy", None),
    )
    out_specs = (P(("chain", "pa"), "gz", "gy", None), P(("chain", "pa"), None))
    return jax.shard_map(shards, mesh=mesh, in_specs=in_specs, out_specs=out_specs, check_vma=False)
```

```python
import functools

import jax
import jax.numpy as jnp
import numpy as np
from jax import lax
from jax.experimental import pallas as pl
from jax.experimental.pallas import tpu as pltpu
from jax.sharding import PartitionSpec as P

MESH = pl.DeviceIdType.MESH
STEPS = 5
SUB = 8

diffuse_cross = 0.15
diffuse_along = 16.0

ZLO, ZHI, YLO, YHI = range(4)
CZP, CZM, CYP, CYM, CXP, CXM, SRC, OBS = range(8)


def implicit_matrix(length):
    banded = (1.0 + 2.0 * diffuse_along) * np.eye(length) - diffuse_along * (
        np.eye(length, k=1) + np.eye(length, k=-1)
    )
    matrix = np.linalg.inv(banded).astype(np.float32)
    high = matrix.astype(jnp.bfloat16)
    low = (matrix - high.astype(np.float32)).astype(jnp.bfloat16)
    return jnp.asarray(high), jnp.asarray(low)


def kernel(
    *refs,
):
    inputs, (hessian_ref, gram_ref), refs = refs[:8], refs[8:10], refs[10:]
    loaded, refs = refs[:8], refs[8:]
    probes_ref, vel_ref, prior_ref, noise_ref, smask_ref, omask_ref, mhi_ref, mlo_ref = loaded
    (
    u_ref,
    s_ref,
    b_ref,
    coef_ref,
    whi_ref,
    wlo_ref,
    zh_ref,
    yh_ref,
    zs_ref,
    ys_ref,
    send_sem,
    recv_sem,
    load_sem,
    out_ref,
    out_sem,
    pu_ref,
    acc_ref,
    sum_ref,
    gt_ref,
    gr_ref,
    pair_send,
    pair_recv,
    tile_send,
    tile_recv,
    ) = refs
    count, nz, ny, nx = probes_ref.shape
    tiles = ny // SUB
    zi, yi = lax.axis_index("gz"), lax.axis_index("gy")
    zn, yn = lax.axis_size("gz"), lax.axis_size("gy")
    exists = [zi > 0, zi < zn - 1, yi > 0, yi < yn - 1]
    target = [
        {"gz": lax.max(zi - 1, 0)},
        {"gz": lax.min(zi + 1, zn - 1)},
        {"gy": lax.max(yi - 1, 0)},
        {"gy": lax.min(yi + 1, yn - 1)},
    ]

    own = lax.axis_index("pa")
    half = nz // 2

    def crossed(me, distance):
        return me + distance * (1 - 2 * ((me // distance) % 2))

    rounds = [{"pa": 1 - own}]
    for axis, me, n in (("gy", yi, yn), ("gz", zi, zn)):
        distance = 1
        while distance < n:
            rounds.append({axis: crossed(me, distance)})
            distance *= 2
    far = 1 if zn > 8 else 0
    z_other = zi - 1 + 2 * (zi % 2)
    y_other = yi - 1 + 2 * (yi % 2)
    met = [
        ((z_other >= 0) & (z_other < zn), {"gz": lax.clamp(0, z_other, zn - 1)}),
        ((y_other >= 0) & (y_other < yn), {"gy": lax.clamp(0, y_other, yn - 1)}),
    ]

    probe_loads = [
        pltpu.make_async_copy(inputs[0].at[p], probes_ref.at[p], load_sem.at[8 + p]) for p in range(count)
    ]
    loads = [None] + [pltpu.make_async_copy(inputs[k], loaded[k], load_sem.at[k]) for k in range(1, 8)]
    for copy in (loads[2], loads[4], probe_loads[0], loads[6], loads[7], *probe_loads[1:]):
        copy.start()
    for copy in (loads[1], loads[3], loads[5]):
        copy.start()

    barrier = pltpu.get_barrier_semaphore()
    greeted = rounds[: len(rounds) - far]
    for device in greeted:
        pl.semaphore_signal(barrier, inc=1, device_id=device, device_id_type=MESH)
    for there, device in met:

        @pl.when(there)
        def _():
            pl.semaphore_signal(barrier, inc=1, device_id=device, device_id_type=MESH)

    row = lax.broadcasted_iota(jnp.int32, (SUB, nx), 0)
    first_row, last_row = row == 0, row == SUB - 1
    lane = lax.broadcasted_iota(jnp.int32, (ny, nx), 1)

    def prepare(z, _):
        vx, vy, vz = (0.5 * vel_ref[c, z] for c in range(3))
        coef_ref[CZP, z] = diffuse_cross - vz
        coef_ref[CZM, z] = diffuse_cross + vz
        coef_ref[CYP, z] = diffuse_cross - vy
        coef_ref[CYM, z] = diffuse_cross + vy
        coef_ref[CXP, z] = jnp.where(lane == nx - 1, 0.0, -vx)
        coef_ref[CXM, z] = jnp.where(lane == 0, 0.0, vx)
        coef_ref[OBS, z] = omask_ref[z].astype(jnp.float32) * noise_ref[z]
        return 0

    @pl.when(zi == 0)
    def _():
        zh_ref[:, 0] = jnp.zeros(zh_ref.shape[:1] + zh_ref.shape[2:], jnp.float32)

    @pl.when(zi == zn - 1)
    def _():
        zh_ref[:, 1] = jnp.zeros(zh_ref.shape[:1] + zh_ref.shape[2:], jnp.float32)

    @pl.when(yi == 0)
    def _():
        yh_ref[:, 0] = jnp.zeros(yh_ref.shape[:1] + yh_ref.shape[2:], jnp.float32)

    @pl.when(yi == yn - 1)
    def _():
        yh_ref[:, 1] = jnp.zeros(yh_ref.shape[:1] + yh_ref.shape[2:], jnp.float32)

    acc_ref[...] = jnp.zeros(acc_ref.shape, jnp.float32)
    loads[2].wait()
    loads[4].wait()
    coef_ref[SRC] = smask_ref[...].astype(jnp.float32) * prior_ref[...]
    loads[6].wait()
    loads[7].wait()
    pl.semaphore_wait(barrier, len(greeted) + sum(there.astype(jnp.int32) for there, _ in met))

    def copies(slot, p, sources):
        result = []
        for side in range(4):
            halo = zh_ref if side < 2 else yh_ref
            result.append(
                pltpu.make_async_remote_copy(
                    src_ref=sources[side],
                    dst_ref=halo.at[slot, (side % 2) ^ 1, p],
                    send_sem=send_sem.at[slot, side, p],
                    recv_sem=recv_sem.at[slot, side ^ 1, p],
                    device_id=target[side],
                    device_id_type=MESH,
                )
            )
        return result

    def send(slot, p, sources):
        for side, copy in enumerate(copies(slot, p, sources)):
            pl.when(exists[side])(copy.start)

    def settle(slot, p, sources):
        moved = copies(slot, p, sources)
        for side in range(4):

            @pl.when(exists[side])
            def _():
                moved[side ^ 1].wait_recv()
                moved[side].wait_send()

    def state_sources(n, slot, p):
        return [u_ref.at[n, p, 0], u_ref.at[n, p, nz - 1], ys_ref.at[slot, 0, p], ys_ref.at[slot, 1, p]]

    def adjoint_sources(slot, p):
        return [zs_ref.at[slot, 0, p], zs_ref.at[slot, 1, p], ys_ref.at[slot, 0, p], ys_ref.at[slot, 1, p]]

    def put(z, pair, left, right):
        rows = jnp.concatenate([left, right], axis=0)
        high = rows.astype(jnp.bfloat16)
        low = (rows - high.astype(jnp.float32)).astype(jnp.bfloat16)
        where = pl.ds(z * ny + pair * 2 * SUB, 2 * SUB)
        whi_ref[where, :] = high
        wlo_ref[where, :] = low

    def solve():
        dot = functools.partial(jnp.dot, preferred_element_type=jnp.float32)
        high, low = whi_ref[...], wlo_ref[...]
        moved = dot(high, mhi_ref[...]) + (dot(high, mlo_ref[...]) + dot(low, mhi_ref[...]))
        return moved.reshape(nz, ny, nx)

    def by_tile(make):
        for z in range(nz):
            for pair in range(tiles // 2):
                put(z, pair, make(z, 2 * pair), make(z, 2 * pair + 1))

    def rows_of(t):
        return pl.ds(t * SUB, SUB)

    def coef(kind, z, t):
        return coef_ref[kind, z, rows_of(t), :]

    def forward(n, slot, p):
        def make(z, t):
            def at(zz, tt):
                return u_ref[n, p, zz, rows_of(tt), :]

            centre = at(z, t)
            plus_z = at(z + 1, t) if z < nz - 1 else zh_ref[slot, 1, p, rows_of(t), :]
            minus_z = at(z - 1, t) if z > 0 else zh_ref[slot, 0, p, rows_of(t), :]
            if t < tiles - 1:
                above = pltpu.roll(at(z, t + 1), SUB - 1, 0)
            else:
                above = jnp.broadcast_to(yh_ref[slot, 1, p, pl.ds(z, 1), :], (SUB, nx))
            if t > 0:
                below = pltpu.roll(at(z, t - 1), 1, 0)
            else:
                below = jnp.broadcast_to(yh_ref[slot, 0, p, pl.ds(z, 1), :], (SUB, nx))
            plus_y = jnp.where(last_row, above, pltpu.roll(centre, SUB - 1, 0))
            minus_y = jnp.where(first_row, below, pltpu.roll(centre, 1, 0))
            total = (1.0 - 4.0 * diffuse_cross) * centre + s_ref[p, z, rows_of(t), :]
            total = total + (coef(CZP, z, t) * plus_z + coef(CZM, z, t) * minus_z)
            total = total + (coef(CYP, z, t) * plus_y + coef(CYM, z, t) * minus_y)
            return total + (
                coef(CXP, z, t) * pltpu.roll(centre, nx - 1, 1) + coef(CXM, z, t) * pltpu.roll(centre, 1, 1)
            )

        by_tile(make)

    def backward(n, slot, p):
        def make(z, t):
            def at(zz, tt):
                return b_ref[p, zz, rows_of(tt), :]

            centre = at(z, t)
            if z < nz - 1:
                plus_z = coef(CZM, z + 1, t) * at(z + 1, t)
            else:
                plus_z = zh_ref[slot, 1, p, rows_of(t), :]
            if z > 0:
                minus_z = coef(CZP, z - 1, t) * at(z - 1, t)
            else:
                minus_z = zh_ref[slot, 0, p, rows_of(t), :]
            if t < tiles - 1:
                above = pltpu.roll(coef(CYM, z, t + 1) * at(z, t + 1), SUB - 1, 0)
            else:
                above = jnp.broadcast_to(yh_ref[slot, 1, p, pl.ds(z, 1), :], (SUB, nx))
            if t > 0:
                below = pltpu.roll(coef(CYP, z, t - 1) * at(z, t - 1), 1, 0)
            else:
                below = jnp.broadcast_to(yh_ref[slot, 0, p, pl.ds(z, 1), :], (SUB, nx))
            plus_y = jnp.where(last_row, above, pltpu.roll(coef(CYM, z, t) * centre, SUB - 1, 0))
            minus_y = jnp.where(first_row, below, pltpu.roll(coef(CYP, z, t) * centre, 1, 0))
            total = (1.0 - 4.0 * diffuse_cross) * centre + coef(OBS, z, t) * u_ref[n, p, z, rows_of(t), :]
            total = total + (plus_z + minus_z)
            total = total + (plus_y + minus_y)
            return total + (
                pltpu.roll(coef(CXM, z, t) * centre, nx - 1, 1) + pltpu.roll(coef(CXP, z, t) * centre, 1, 1)
            )

        by_tile(make)

    def finish_state(n, slot, p):
        state = solve()
        u_ref[n, p] = state
        for z in range(nz):
            ys_ref[slot, 0, p, pl.ds(z, 1), :] = state[z, 0:1, :]
            ys_ref[slot, 1, p, pl.ds(z, 1), :] = state[z, ny - 1 : ny, :]

    def finish_adjoint(slot, p, pulled):
        b_ref[p] = pulled
        zs_ref[slot, 0, p] = coef_ref[CZM, 0] * pulled[0]
        zs_ref[slot, 1, p] = coef_ref[CZP, nz - 1] * pulled[nz - 1]
        for z in range(nz):
            ys_ref[slot, 0, p, pl.ds(z, 1), :] = coef_ref[CYM, z, 0:1, :] * pulled[z, 0:1, :]
            ys_ref[slot, 1, p, pl.ds(z, 1), :] = coef_ref[CYP, z, ny - 1 : ny, :] * pulled[z, ny - 1 : ny, :]

    def pair_copy(n):
        return pltpu.make_async_remote_copy(
            src_ref=u_ref.at[n, :, pl.ds((1 - own) * half, half)],
            dst_ref=pu_ref.at[n],
            send_sem=pair_send.at[n],
            recv_sem=pair_recv.at[n],
            device_id=rounds[0],
            device_id_type=MESH,
        )

    def tile_copy(k):
        return pltpu.make_async_remote_copy(
            src_ref=gt_ref.at[k if k == 0 else k + 1],
            dst_ref=gr_ref.at[k],
            send_sem=tile_send.at[k],
            recv_sem=tile_recv.at[k],
            device_id=rounds[k],
            device_id_type=MESH,
        )

    near = count // 2 + 1
    lanes = 128
    pieces = [(t, h) for t in range(tiles) for h in range(nx // lanes)]

    def gram_unit(n, i):
        if count != 8:
            raise NotImplementedError
        wait_pair = pl.when(i == 0)

        @wait_pair
        def _():
            pair_copy(n).wait()

        def own_terms(z, sums):
            sums = list(sums)
            for t, h in pieces:
                where = (rows_of(t), pl.ds(h * lanes, lanes))
                x = [u_ref[(n, (i + d) % count, z) + where] for d in range(near + 1)]
                weight = coef_ref[(OBS, z) + where]
                for r in range(2):
                    scaled = weight * x[r]
                    for d in range(near):
                        sums[r * near + d] = sums[r * near + d] + scaled * x[r + d]
            return tuple(sums)

        def pair_terms(z, sums):
            sums = list(sums)
            for t, h in pieces:
                where = (rows_of(t), pl.ds(h * lanes, lanes))
                weight = coef_ref[(OBS, own * half + z) + where]
                scaled = [weight * u_ref[(n, i + r, own * half + z) + where] for r in range(2)]
                for j in range(count):
                    y = pu_ref[(n, j, z) + where]
                    for r in range(2):
                        sums[r * count + j] = sums[r * count + j] + scaled[r] * y
            return tuple(sums)

        zero = jnp.zeros((SUB, lanes), jnp.float32)
        sums = lax.fori_loop(0, nz, own_terms, (zero,) * (2 * near))
        for r in range(2):
            for d in range(near):
                acc_ref[i + r, d] += sums[r * near + d]
        sums = lax.fori_loop(0, half, pair_terms, (zero,) * (2 * count))
        for r in range(2):
            for j in range(count):
                acc_ref[i + r, near + j] += sums[r * count + j]

    def gram_tile():
        ones = jnp.ones((lanes, lanes), jnp.float32)
        kinds = near + count

        def by_lanes(i, _):
            partial = acc_ref[i].reshape(kinds * SUB, lanes)
            total = jnp.dot(
                partial, ones, precision=lax.Precision.HIGHEST, preferred_element_type=jnp.float32
            )
            sum_ref[i] = total.reshape(kinds, SUB, lanes)
            return 0

        lax.fori_loop(0, count, by_lanes, 0)
        at_row = lax.broadcasted_iota(jnp.int32, (SUB, lanes), 0)
        at_lane = lax.broadcasted_iota(jnp.int32, (SUB, lanes), 1)
        mine, theirs = at_lane - own * count, at_lane - (1 - own) * count
        tile = jnp.zeros((SUB, lanes), jnp.float32)
        sent = jnp.zeros((SUB, lanes), jnp.float32)
        for i in range(count):
            for k in range(kinds):
                value = sum_ref[i, k]
                for shift in (4, 2, 1):
                    value = value + pltpu.roll(value, shift, 0)
                if k < near:
                    j = (i + k) % count
                    here = (at_row == i) & (mine == j)
                    if 0 < k < near - 1:
                        here = here | ((at_row == j) & (mine == i))
                    tile = tile + jnp.where(here, value, 0.0)
                else:
                    j = k - near
                    tile = tile + jnp.where((at_row == i) & (theirs == j), value, 0.0)
                    sent = sent + jnp.where((at_row == j) & (mine == i), value, 0.0)
        gt_ref[0] = sent
        gt_ref[1] = tile

    def gram_round(k):
        tile_copy(k).wait()
        gt_ref[k + 2] = gt_ref[k + 1] + gr_ref[k]
        if k + 1 < len(rounds):
            tile_copy(k + 1).start()

    round_ends = (7, 9, 12, 14, 17, 22)

    def out_copy(p):
        return pltpu.make_async_copy(out_ref.at[p], hessian_ref.at[p], out_sem.at[p])

    last = STEPS - 1

    def first_step(p, _):
        pltpu.make_async_copy(inputs[0].at[p], probes_ref.at[p], load_sem.at[8 + p]).wait()
        for z in range(nz):
            for t in range(tiles):
                s_ref[p, z, rows_of(t), :] = coef(SRC, z, t) * probes_ref[p, z, rows_of(t), :]
        by_tile(lambda z, t: coef(SRC, z, t) * probes_ref[p, z, rows_of(t), :])
        finish_state(0, 0, p)
        send(0, p, state_sources(0, 0, p))
        return 0

    lax.fori_loop(0, count, first_step, 0)
    pair_copy(0).start()
    for k in (1, 3, 5):
        loads[k].wait()
    lax.fori_loop(0, nz, prepare, 0)

    def forward_step(i, _):
        n, p = i // count + 1, i % count
        before, now = (n + 1) % 2, n % 2
        settle(before, p, state_sources(n - 1, before, p))
        forward(n - 1, before, p)
        finish_state(n, now, p)
        send(now, p, state_sources(n, now, p))

        @pl.when(p == count - 1)
        def _():
            pair_copy(n).start()

        @pl.when(p % 2 == 1)
        def _():
            gram_unit(n - 1, p - 1)

        return 0

    lax.fori_loop(0, (last - 1) * count, forward_step, 0)

    def turn_step(p, _):
        before, now = (last + 1) % 2, last % 2
        settle(before, p, state_sources(last - 1, before, p))
        forward(last - 1, before, p)
        u_ref[last, p] = solve()
        by_tile(lambda z, t: coef(OBS, z, t) * u_ref[last, p, z, rows_of(t), :])
        pulled = solve()
        out_ref[p] = pulled
        finish_adjoint(now, p, pulled)
        send(now, p, adjoint_sources(now, p))

        @pl.when(p % 2 == 1)
        def _():
            gram_unit(last - 1, p - 1)

        return 0

    lax.fori_loop(0, count, turn_step, 0)
    pair_copy(last).start()

    def backward_step(i, _):
        k, p = i // count + 1, i % count
        before, now = (last + k + 1) % 2, (last + k) % 2
        settle(before, p, adjoint_sources(before, p))
        backward(last - k, before, p)
        pulled = solve()
        out_ref[p] += pulled
        finish_adjoint(now, p, pulled)
        send(now, p, adjoint_sources(now, p))

        @pl.when((i >= 2) & (i < 6))
        def _():
            gram_unit(last, 2 * (i - 2))

        @pl.when(i == 5)
        def _():
            gram_tile()
            tile_copy(0).start()

        for k, end in enumerate(round_ends[: len(rounds)]):

            @pl.when(i == end)
            def _():
                gram_round(k)

        return 0

    lax.fori_loop(0, (last - 1) * count, backward_step, 0)

    def last_step(p, _):
        before = (2 * last + 1) % 2
        settle(before, p, adjoint_sources(before, p))
        backward(0, before, p)
        out_ref[p] = coef_ref[SRC] * (out_ref[p] + solve())
        out_copy(p).start()
        return 0

    lax.fori_loop(0, count, last_step, 0)
    for k in range(len(round_ends), len(rounds)):
        gram_round(k)
    for p in range(count):
        out_copy(p).wait()
    gram_ref[...] = gt_ref[len(rounds) + 1, :, : gram_ref.shape[1]] / (nz * ny * nx * zn * yn)


def shards(probes, velocity, prior_scale, noise_precision, source_mask, sensor_mask):
    count, nz, ny, nx = probes.shape
    high, low = implicit_matrix(nx)
    arguments = (probes, velocity, prior_scale, noise_precision, source_mask, sensor_mask, high, low)
    cores = lax.axis_size("pa")
    rounds = 1 + (lax.axis_size("gy") - 1).bit_length() + (lax.axis_size("gz") - 1).bit_length()
    near = count // 2 + 1
    return pl.pallas_call(
        kernel,
        out_shape=(
            jax.ShapeDtypeStruct(probes.shape, jnp.float32),
            jax.ShapeDtypeStruct((count, cores * count), jnp.float32),
        ),
        in_specs=[pl.BlockSpec(memory_space=pltpu.HBM)] * len(arguments),
        out_specs=(pl.BlockSpec(memory_space=pltpu.HBM), pl.BlockSpec(memory_space=pltpu.VMEM)),
        scratch_shapes=[
            *(pltpu.VMEM(array.shape, array.dtype) for array in arguments),
            pltpu.VMEM((STEPS, count, nz, ny, nx), jnp.float32),
            pltpu.VMEM((count, nz, ny, nx), jnp.float32),
            pltpu.VMEM((count, nz, ny, nx), jnp.float32),
            pltpu.VMEM((8, nz, ny, nx), jnp.float32),
            pltpu.VMEM((nz * ny, nx), jnp.bfloat16),
            pltpu.VMEM((nz * ny, nx), jnp.bfloat16),
            pltpu.VMEM((2, 2, count, ny, nx), jnp.float32),
            pltpu.VMEM((2, 2, count, nz, nx), jnp.float32),
            pltpu.VMEM((2, 2, count, ny, nx), jnp.float32),
            pltpu.VMEM((2, 2, count, nz, nx), jnp.float32),
            pltpu.SemaphoreType.DMA((2, 4, count)),
            pltpu.SemaphoreType.DMA((2, 4, count)),
            pltpu.SemaphoreType.DMA((8 + count,)),
            pltpu.VMEM((count, nz, ny, nx), jnp.float32),
            pltpu.SemaphoreType.DMA((count,)),
            pltpu.VMEM((STEPS, count, nz // 2, ny, nx), jnp.float32),
            pltpu.VMEM((count, near + count, SUB, 128), jnp.float32),
            pltpu.VMEM((count, near + count, SUB, 128), jnp.float32),
            pltpu.VMEM((rounds + 2, SUB, 128), jnp.float32),
            pltpu.VMEM((rounds, SUB, 128), jnp.float32),
            pltpu.SemaphoreType.DMA((STEPS,)),
            pltpu.SemaphoreType.DMA((STEPS,)),
            pltpu.SemaphoreType.DMA((rounds,)),
            pltpu.SemaphoreType.DMA((rounds,)),
        ],
        compiler_params=pltpu.CompilerParams(
            collective_id=0, has_side_effects=True, vmem_limit_bytes=60 * 1024 * 1024
        ),
        name="solve",
    )(*arguments)


def solution(mesh):
    in_specs = (
        P(("chain", "pa"), "gz", "gy", None),
        P(None, ("chain", "gz"), "gy", None),
        P(("chain", "gz"), "gy", None),
        P(("chain", "gz"), "gy", None),
        P(("chain", "gz"), "gy", None),
        P(("chain", "gz"), "gy", None),
    )
    out_specs = (P(("chain", "pa"), "gz", "gy", None), P(("chain", "pa"), None))
    return jax.shard_map(shards, mesh=mesh, in_specs=in_specs, out_specs=out_specs, check_vma=False)
```

```python
import functools

import jax
import jax.numpy as jnp
import numpy as np
from jax import lax
from jax.experimental import pallas as pl
from jax.experimental.pallas import tpu as pltpu
from jax.sharding import PartitionSpec as P

MESH = pl.DeviceIdType.MESH
STEPS = 5
SUB = 8

diffuse_cross = 0.15
diffuse_along = 16.0

ZLO, ZHI, YLO, YHI = range(4)
CZP, CZM, CYP, CYM, CXP, CXM, SRC, OBS = range(8)


def implicit_matrix(length):
    banded = (1.0 + 2.0 * diffuse_along) * np.eye(length) - diffuse_along * (
        np.eye(length, k=1) + np.eye(length, k=-1)
    )
    matrix = np.linalg.inv(banded).astype(np.float32)
    high = matrix.astype(jnp.bfloat16)
    low = (matrix - high.astype(np.float32)).astype(jnp.bfloat16)
    return jnp.asarray(high), jnp.asarray(low)


def kernel(
    *refs,
):
    inputs, (hessian_ref, gram_ref), refs = refs[:8], refs[8:10], refs[10:]
    loaded, refs = refs[:8], refs[8:]
    probes_ref, vel_ref, prior_ref, noise_ref, smask_ref, omask_ref, mhi_ref, mlo_ref = loaded
    (
    u_ref,
    s_ref,
    b_ref,
    coef_ref,
    whi_ref,
    wlo_ref,
    zh_ref,
    yh_ref,
    zs_ref,
    ys_ref,
    send_sem,
    recv_sem,
    load_sem,
    out_ref,
    out_sem,
    pu_ref,
    acc_ref,
    sum_ref,
    gt_ref,
    gr_ref,
    pair_send,
    pair_recv,
    ys_sem,
    yr_sem,
    zs_sem,
    zr_sem,
    core_sem,
    word_sem,
    ytile_ref,
    ztile_ref,
    ) = refs
    count, nz, ny, nx = probes_ref.shape
    tiles = ny // SUB
    zi, yi = lax.axis_index("gz"), lax.axis_index("gy")
    zn, yn = lax.axis_size("gz"), lax.axis_size("gy")
    exists = [zi > 0, zi < zn - 1, yi > 0, yi < yn - 1]
    target = [
        {"gz": lax.max(zi - 1, 0)},
        {"gz": lax.min(zi + 1, zn - 1)},
        {"gy": lax.max(yi - 1, 0)},
        {"gy": lax.min(yi + 1, yn - 1)},
    ]

    own = lax.axis_index("pa")
    half = nz // 2

    def crossed(me, distance):
        return me + distance * (1 - 2 * ((me // distance) % 2))

    def doubled(axis, me, n):
        return [{axis: crossed(me, 1 << k)} for k in range((n - 1).bit_length())]

    other_core = {"pa": 1 - own}
    y_doubled, z_doubled = doubled("gy", yi, yn), doubled("gz", zi, zn)
    z_other = zi - 1 + 2 * (zi % 2)
    y_other = yi - 1 + 2 * (yi % 2)
    met = [
        ((z_other >= 0) & (z_other < zn), {"gz": lax.clamp(0, z_other, zn - 1)}),
        ((y_other >= 0) & (y_other < yn), {"gy": lax.clamp(0, y_other, yn - 1)}),
    ]

    probe_loads = [
        pltpu.make_async_copy(inputs[0].at[p], probes_ref.at[p], load_sem.at[8 + p]) for p in range(count)
    ]
    loads = [None] + [pltpu.make_async_copy(inputs[k], loaded[k], load_sem.at[k]) for k in range(1, 8)]
    for copy in (loads[2], loads[4], probe_loads[0], loads[6], loads[7], *probe_loads[1:]):
        copy.start()
    for copy in (loads[1], loads[3], loads[5]):
        copy.start()

    barrier = pltpu.get_barrier_semaphore()
    greeted = [other_core] + y_doubled + z_doubled[:3]
    for device in greeted:
        pl.semaphore_signal(barrier, inc=1, device_id=device, device_id_type=MESH)
    for there, device in met:

        @pl.when(there)
        def _():
            pl.semaphore_signal(barrier, inc=1, device_id=device, device_id_type=MESH)

    row = lax.broadcasted_iota(jnp.int32, (SUB, nx), 0)
    first_row, last_row = row == 0, row == SUB - 1
    lane = lax.broadcasted_iota(jnp.int32, (ny, nx), 1)

    def prepare(z, _):
        vx, vy, vz = (0.5 * vel_ref[c, z] for c in range(3))
        coef_ref[CZP, z] = diffuse_cross - vz
        coef_ref[CZM, z] = diffuse_cross + vz
        coef_ref[CYP, z] = diffuse_cross - vy
        coef_ref[CYM, z] = diffuse_cross + vy
        coef_ref[CXP, z] = jnp.where(lane == nx - 1, 0.0, -vx)
        coef_ref[CXM, z] = jnp.where(lane == 0, 0.0, vx)
        coef_ref[OBS, z] = omask_ref[z].astype(jnp.float32) * noise_ref[z]
        return 0

    @pl.when(zi == 0)
    def _():
        zh_ref[:, 0] = jnp.zeros(zh_ref.shape[:1] + zh_ref.shape[2:], jnp.float32)

    @pl.when(zi == zn - 1)
    def _():
        zh_ref[:, 1] = jnp.zeros(zh_ref.shape[:1] + zh_ref.shape[2:], jnp.float32)

    @pl.when(yi == 0)
    def _():
        yh_ref[:, 0] = jnp.zeros(yh_ref.shape[:1] + yh_ref.shape[2:], jnp.float32)

    @pl.when(yi == yn - 1)
    def _():
        yh_ref[:, 1] = jnp.zeros(yh_ref.shape[:1] + yh_ref.shape[2:], jnp.float32)

    acc_ref[...] = jnp.zeros(acc_ref.shape, jnp.float32)
    loads[2].wait()
    loads[4].wait()
    coef_ref[SRC] = smask_ref[...].astype(jnp.float32) * prior_ref[...]
    loads[6].wait()
    loads[7].wait()
    pl.semaphore_wait(barrier, len(greeted) + sum(there.astype(jnp.int32) for there, _ in met))

    def copies(slot, p, sources):
        result = []
        for side in range(4):
            halo = zh_ref if side < 2 else yh_ref
            result.append(
                pltpu.make_async_remote_copy(
                    src_ref=sources[side],
                    dst_ref=halo.at[slot, (side % 2) ^ 1, p],
                    send_sem=send_sem.at[slot, side, p],
                    recv_sem=recv_sem.at[slot, side ^ 1, p],
                    device_id=target[side],
                    device_id_type=MESH,
                )
            )
        return result

    def send(slot, p, sources):
        for side, copy in enumerate(copies(slot, p, sources)):
            pl.when(exists[side])(copy.start)

    def settle(slot, p, sources):
        moved = copies(slot, p, sources)
        for side in range(4):

            @pl.when(exists[side])
            def _():
                moved[side ^ 1].wait_recv()
                moved[side].wait_send()

    def state_sources(n, slot, p):
        return [u_ref.at[n, p, 0], u_ref.at[n, p, nz - 1], ys_ref.at[slot, 0, p], ys_ref.at[slot, 1, p]]

    def adjoint_sources(slot, p):
        return [zs_ref.at[slot, 0, p], zs_ref.at[slot, 1, p], ys_ref.at[slot, 0, p], ys_ref.at[slot, 1, p]]

    def put(z, pair, left, right):
        rows = jnp.concatenate([left, right], axis=0)
        high = rows.astype(jnp.bfloat16)
        low = (rows - high.astype(jnp.float32)).astype(jnp.bfloat16)
        where = pl.ds(z * ny + pair * 2 * SUB, 2 * SUB)
        whi_ref[where, :] = high
        wlo_ref[where, :] = low

    def solve():
        dot = functools.partial(jnp.dot, preferred_element_type=jnp.float32)
        high, low = whi_ref[...], wlo_ref[...]
        moved = dot(high, mhi_ref[...]) + (dot(high, mlo_ref[...]) + dot(low, mhi_ref[...]))
        return moved.reshape(nz, ny, nx)

    def by_tile(make):
        for z in range(nz):
            for pair in range(tiles // 2):
                put(z, pair, make(z, 2 * pair), make(z, 2 * pair + 1))

    def rows_of(t):
        return pl.ds(t * SUB, SUB)

    def coef(kind, z, t):
        return coef_ref[kind, z, rows_of(t), :]

    def forward(n, slot, p):
        def make(z, t):
            def at(zz, tt):
                return u_ref[n, p, zz, rows_of(tt), :]

            centre = at(z, t)
            plus_z = at(z + 1, t) if z < nz - 1 else zh_ref[slot, 1, p, rows_of(t), :]
            minus_z = at(z - 1, t) if z > 0 else zh_ref[slot, 0, p, rows_of(t), :]
            if t < tiles - 1:
                above = pltpu.roll(at(z, t + 1), SUB - 1, 0)
            else:
                above = jnp.broadcast_to(yh_ref[slot, 1, p, pl.ds(z, 1), :], (SUB, nx))
            if t > 0:
                below = pltpu.roll(at(z, t - 1), 1, 0)
            else:
                below = jnp.broadcast_to(yh_ref[slot, 0, p, pl.ds(z, 1), :], (SUB, nx))
            plus_y = jnp.where(last_row, above, pltpu.roll(centre, SUB - 1, 0))
            minus_y = jnp.where(first_row, below, pltpu.roll(centre, 1, 0))
            total = (1.0 - 4.0 * diffuse_cross) * centre + s_ref[p, z, rows_of(t), :]
            total = total + (coef(CZP, z, t) * plus_z + coef(CZM, z, t) * minus_z)
            total = total + (coef(CYP, z, t) * plus_y + coef(CYM, z, t) * minus_y)
            return total + (
                coef(CXP, z, t) * pltpu.roll(centre, nx - 1, 1) + coef(CXM, z, t) * pltpu.roll(centre, 1, 1)
            )

        by_tile(make)

    def backward(n, slot, p):
        def make(z, t):
            def at(zz, tt):
                return b_ref[p, zz, rows_of(tt), :]

            centre = at(z, t)
            if z < nz - 1:
                plus_z = coef(CZM, z + 1, t) * at(z + 1, t)
            else:
                plus_z = zh_ref[slot, 1, p, rows_of(t), :]
            if z > 0:
                minus_z = coef(CZP, z - 1, t) * at(z - 1, t)
            else:
                minus_z = zh_ref[slot, 0, p, rows_of(t), :]
            if t < tiles - 1:
                above = pltpu.roll(coef(CYM, z, t + 1) * at(z, t + 1), SUB - 1, 0)
            else:
                above = jnp.broadcast_to(yh_ref[slot, 1, p, pl.ds(z, 1), :], (SUB, nx))
            if t > 0:
                below = pltpu.roll(coef(CYP, z, t - 1) * at(z, t - 1), 1, 0)
            else:
                below = jnp.broadcast_to(yh_ref[slot, 0, p, pl.ds(z, 1), :], (SUB, nx))
            plus_y = jnp.where(last_row, above, pltpu.roll(coef(CYM, z, t) * centre, SUB - 1, 0))
            minus_y = jnp.where(first_row, below, pltpu.roll(coef(CYP, z, t) * centre, 1, 0))
            total = (1.0 - 4.0 * diffuse_cross) * centre + coef(OBS, z, t) * u_ref[n, p, z, rows_of(t), :]
            total = total + (plus_z + minus_z)
            total = total + (plus_y + minus_y)
            return total + (
                pltpu.roll(coef(CXM, z, t) * centre, nx - 1, 1) + pltpu.roll(coef(CXP, z, t) * centre, 1, 1)
            )

        by_tile(make)

    def finish_state(n, slot, p):
        state = solve()
        u_ref[n, p] = state
        for z in range(nz):
            ys_ref[slot, 0, p, pl.ds(z, 1), :] = state[z, 0:1, :]
            ys_ref[slot, 1, p, pl.ds(z, 1), :] = state[z, ny - 1 : ny, :]

    def finish_adjoint(slot, p, pulled):
        b_ref[p] = pulled
        zs_ref[slot, 0, p] = coef_ref[CZM, 0] * pulled[0]
        zs_ref[slot, 1, p] = coef_ref[CZP, nz - 1] * pulled[nz - 1]
        for z in range(nz):
            ys_ref[slot, 0, p, pl.ds(z, 1), :] = coef_ref[CYM, z, 0:1, :] * pulled[z, 0:1, :]
            ys_ref[slot, 1, p, pl.ds(z, 1), :] = coef_ref[CYP, z, ny - 1 : ny, :] * pulled[z, ny - 1 : ny, :]

    def pair_copy(n):
        return pltpu.make_async_remote_copy(
            src_ref=u_ref.at[n, :, pl.ds((1 - own) * half, half)],
            dst_ref=pu_ref.at[n],
            send_sem=pair_send.at[n],
            recv_sem=pair_recv.at[n],
            device_id=other_core,
            device_id_type=MESH,
        )

    def core_tile():
        return pltpu.make_async_remote_copy(
            src_ref=gt_ref.at[0],
            dst_ref=gr_ref,
            send_sem=core_sem.at[0],
            recv_sem=core_sem.at[1],
            device_id=other_core,
            device_id_type=MESH,
        )

    def along(axis, me, n, tiles_ref, source, out_sem, in_sem):
        def move(distance):
            return pltpu.make_async_remote_copy(
                src_ref=source,
                dst_ref=tiles_ref.at[me],
                send_sem=out_sem.at[distance],
                recv_sem=in_sem.at[me],
                device_id={axis: (me + distance) % n},
                device_id_type=MESH,
            )

        def arrival(who):
            return pltpu.make_async_remote_copy(
                src_ref=source,
                dst_ref=tiles_ref.at[who],
                send_sem=out_sem.at[0],
                recv_sem=in_sem.at[who],
                device_id={axis: (me + 1) % n},
                device_id_type=MESH,
            )

        def start():
            def step(distance, _):
                move(distance).start()
                return 0

            lax.fori_loop(1, n, step, 0)

        def end():
            def step(distance, _):
                arrival((me + distance) % n).wait_recv()
                move(distance).wait_send()
                return 0

            lax.fori_loop(1, n, step, 0)
            tiles_ref[me] = source[...]
            total = tiles_ref[0]
            for who in range(1, n):
                total = total + tiles_ref[who]
            return total

        return start, end

    start_y, end_y = along("gy", yi, yn, ytile_ref, gt_ref.at[2], ys_sem, yr_sem)
    start_z, end_z = along("gz", zi, zn, ztile_ref, gt_ref.at[3], zs_sem, zr_sem)

    def pass_word(k):
        if 0 < k <= len(z_doubled[:3]):
            pl.semaphore_wait(word_sem.at[k - 1], 1)
        if k < len(z_doubled[:3]):
            pl.semaphore_signal(word_sem.at[k], inc=1, device_id=z_doubled[k], device_id_type=MESH)

    near = count // 2 + 1
    lanes = 128
    pieces = [(t, h) for t in range(tiles) for h in range(nx // lanes)]

    def gram_unit(n, i):
        if count != 8:
            raise NotImplementedError
        wait_pair = pl.when(i == 0)

        @wait_pair
        def _():
            pair_copy(n).wait()

        def own_terms(k, sums):
            sums = list(sums)
            for z in (2 * k, 2 * k + 1):
                for t, h in pieces:
                    where = (rows_of(t), pl.ds(h * lanes, lanes))
                    x = [u_ref[(n, (i + d) % count, z) + where] for d in range(near + 1)]
                    weight = coef_ref[(OBS, z) + where]
                    for r in range(2):
                        scaled = weight * x[r]
                        for d in range(near):
                            sums[r * near + d] = sums[r * near + d] + scaled * x[r + d]
            return tuple(sums)

        def pair_terms(k, sums):
            sums = list(sums)
            for z in (2 * k, 2 * k + 1):
                for t, h in pieces:
                    where = (rows_of(t), pl.ds(h * lanes, lanes))
                    weight = coef_ref[(OBS, own * half + z) + where]
                    scaled = [weight * u_ref[(n, i + r, own * half + z) + where] for r in range(2)]
                    for j in range(count):
                        y = pu_ref[(n, j, z) + where]
                        for r in range(2):
                            sums[r * count + j] = sums[r * count + j] + scaled[r] * y
            return tuple(sums)

        zero = jnp.zeros((SUB, lanes), jnp.float32)
        sums = lax.fori_loop(0, nz // 2, own_terms, (zero,) * (2 * near))
        for r in range(2):
            for d in range(near):
                acc_ref[i + r, d] += sums[r * near + d]
        sums = lax.fori_loop(0, half // 2, pair_terms, (zero,) * (2 * count))
        for r in range(2):
            for j in range(count):
                acc_ref[i + r, near + j] += sums[r * count + j]

    def gram_tile():
        ones = jnp.ones((lanes, lanes), jnp.float32)
        kinds = near + count

        def by_lanes(i, _):
            partial = acc_ref[i].reshape(kinds * SUB, lanes)
            total = jnp.dot(
                partial, ones, precision=lax.Precision.HIGHEST, preferred_element_type=jnp.float32
            )
            sum_ref[i] = total.reshape(kinds, SUB, lanes)
            return 0

        lax.fori_loop(0, count, by_lanes, 0)
        at_row = lax.broadcasted_iota(jnp.int32, (SUB, lanes), 0)
        at_lane = lax.broadcasted_iota(jnp.int32, (SUB, lanes), 1)
        mine, theirs = at_lane - own * count, at_lane - (1 - own) * count
        tile = jnp.zeros((SUB, lanes), jnp.float32)
        sent = jnp.zeros((SUB, lanes), jnp.float32)
        for i in range(count):
            for k in range(kinds):
                value = sum_ref[i, k]
                for shift in (4, 2, 1):
                    value = value + pltpu.roll(value, shift, 0)
                if k < near:
                    j = (i + k) % count
                    here = (at_row == i) & (mine == j)
                    if 0 < k < near - 1:
                        here = here | ((at_row == j) & (mine == i))
                    tile = tile + jnp.where(here, value, 0.0)
                else:
                    j = k - near
                    tile = tile + jnp.where((at_row == i) & (theirs == j), value, 0.0)
                    sent = sent + jnp.where((at_row == j) & (mine == i), value, 0.0)
        gt_ref[0] = sent
        gt_ref[1] = tile

    def end_core():
        core_tile().wait()
        gt_ref[2] = gt_ref[1] + gr_ref[...]
        start_y()

    def end_rows():
        gt_ref[3] = end_y()
        start_z()

    def out_copy(p):
        return pltpu.make_async_copy(out_ref.at[p], hessian_ref.at[p], out_sem.at[p])

    last = STEPS - 1

    def first_step(p, _):
        pltpu.make_async_copy(inputs[0].at[p], probes_ref.at[p], load_sem.at[8 + p]).wait()
        for z in range(nz):
            for t in range(tiles):
                s_ref[p, z, rows_of(t), :] = coef(SRC, z, t) * probes_ref[p, z, rows_of(t), :]
        by_tile(lambda z, t: coef(SRC, z, t) * probes_ref[p, z, rows_of(t), :])
        finish_state(0, 0, p)
        send(0, p, state_sources(0, 0, p))
        return 0

    lax.fori_loop(0, count, first_step, 0)
    pair_copy(0).start()
    for k in (1, 3, 5):
        loads[k].wait()
    lax.fori_loop(0, nz, prepare, 0)

    def forward_step(i, _):
        n, p = i // count + 1, i % count
        before, now = (n + 1) % 2, n % 2
        settle(before, p, state_sources(n - 1, before, p))
        forward(n - 1, before, p)
        finish_state(n, now, p)
        send(now, p, state_sources(n, now, p))

        @pl.when(p == count - 1)
        def _():
            pair_copy(n).start()

        @pl.when(p % 2 == 1)
        def _():
            gram_unit(n - 1, p - 1)

        return 0

    lax.fori_loop(0, (last - 1) * count, forward_step, 0)

    def turn_step(p, _):
        before, now = (last + 1) % 2, last % 2
        settle(before, p, state_sources(last - 1, before, p))
        forward(last - 1, before, p)
        u_ref[last, p] = solve()
        by_tile(lambda z, t: coef(OBS, z, t) * u_ref[last, p, z, rows_of(t), :])
        pulled = solve()
        out_ref[p] = pulled
        finish_adjoint(now, p, pulled)
        send(now, p, adjoint_sources(now, p))

        @pl.when(p % 2 == 1)
        def _():
            gram_unit(last - 1, p - 1)

        return 0

    lax.fori_loop(0, count, turn_step, 0)
    pair_copy(last).start()
    pass_word(0)

    def backward_step(i, _):
        k, p = i // count + 1, i % count
        before, now = (last + k + 1) % 2, (last + k) % 2
        settle(before, p, adjoint_sources(before, p))
        backward(last - k, before, p)
        pulled = solve()
        out_ref[p] += pulled
        finish_adjoint(now, p, pulled)
        send(now, p, adjoint_sources(now, p))

        @pl.when((i >= 2) & (i < 6))
        def _():
            gram_unit(last, 2 * (i - 2))

        for k, when in enumerate((1, 4, 8)):

            @pl.when(i == when)
            def _():
                pass_word(k + 1)

        @pl.when(i == 5)
        def _():
            gram_tile()
            core_tile().start()

        pl.when(i == 7)(end_core)
        pl.when(i == 10)(end_rows)
        return 0

    lax.fori_loop(0, (last - 1) * count, backward_step, 0)

    def last_step(p, _):
        before = (2 * last + 1) % 2
        settle(before, p, adjoint_sources(before, p))
        backward(0, before, p)
        out_ref[p] = coef_ref[SRC] * (out_ref[p] + solve())
        out_copy(p).start()
        return 0

    lax.fori_loop(0, count, last_step, 0)
    for p in range(count):
        out_copy(p).wait()
    gram_ref[...] = end_z()[:, : gram_ref.shape[1]] / (nz * ny * nx * zn * yn)


def shards(probes, velocity, prior_scale, noise_precision, source_mask, sensor_mask):
    count, nz, ny, nx = probes.shape
    high, low = implicit_matrix(nx)
    arguments = (probes, velocity, prior_scale, noise_precision, source_mask, sensor_mask, high, low)
    cores = lax.axis_size("pa")
    zn, yn = lax.axis_size("gz"), lax.axis_size("gy")
    near = count // 2 + 1
    return pl.pallas_call(
        kernel,
        out_shape=(
            jax.ShapeDtypeStruct(probes.shape, jnp.float32),
            jax.ShapeDtypeStruct((count, cores * count), jnp.float32),
        ),
        in_specs=[pl.BlockSpec(memory_space=pltpu.HBM)] * len(arguments),
        out_specs=(pl.BlockSpec(memory_space=pltpu.HBM), pl.BlockSpec(memory_space=pltpu.VMEM)),
        scratch_shapes=[
            *(pltpu.VMEM(array.shape, array.dtype) for array in arguments),
            pltpu.VMEM((STEPS, count, nz, ny, nx), jnp.float32),
            pltpu.VMEM((count, nz, ny, nx), jnp.float32),
            pltpu.VMEM((count, nz, ny, nx), jnp.float32),
            pltpu.VMEM((8, nz, ny, nx), jnp.float32),
            pltpu.VMEM((nz * ny, nx), jnp.bfloat16),
            pltpu.VMEM((nz * ny, nx), jnp.bfloat16),
            pltpu.VMEM((2, 2, count, ny, nx), jnp.float32),
            pltpu.VMEM((2, 2, count, nz, nx), jnp.float32),
            pltpu.VMEM((2, 2, count, ny, nx), jnp.float32),
            pltpu.VMEM((2, 2, count, nz, nx), jnp.float32),
            pltpu.SemaphoreType.DMA((2, 4, count)),
            pltpu.SemaphoreType.DMA((2, 4, count)),
            pltpu.SemaphoreType.DMA((8 + count,)),
            pltpu.VMEM((count, nz, ny, nx), jnp.float32),
            pltpu.SemaphoreType.DMA((count,)),
            pltpu.VMEM((STEPS, count, nz // 2, ny, nx), jnp.float32),
            pltpu.VMEM((count, near + count, SUB, 128), jnp.float32),
            pltpu.VMEM((count, near + count, SUB, 128), jnp.float32),
            pltpu.VMEM((4, SUB, 128), jnp.float32),
            pltpu.VMEM((SUB, 128), jnp.float32),
            pltpu.SemaphoreType.DMA((STEPS,)),
            pltpu.SemaphoreType.DMA((STEPS,)),
            pltpu.SemaphoreType.DMA((yn,)),
            pltpu.SemaphoreType.DMA((yn,)),
            pltpu.SemaphoreType.DMA((zn,)),
            pltpu.SemaphoreType.DMA((zn,)),
            pltpu.SemaphoreType.DMA((2,)),
            pltpu.SemaphoreType.REGULAR((3,)),
            pltpu.VMEM((yn, SUB, 128), jnp.float32),
            pltpu.VMEM((zn, SUB, 128), jnp.float32),
        ],
        compiler_params=pltpu.CompilerParams(
            collective_id=0, has_side_effects=True, vmem_limit_bytes=60 * 1024 * 1024
        ),
        name="solve",
    )(*arguments)


def solution(mesh):
    in_specs = (
        P(("chain", "pa"), "gz", "gy", None),
        P(None, ("chain", "gz"), "gy", None),
        P(("chain", "gz"), "gy", None),
        P(("chain", "gz"), "gy", None),
        P(("chain", "gz"), "gy", None),
        P(("chain", "gz"), "gy", None),
    )
    out_specs = (P(("chain", "pa"), "gz", "gy", None), P(("chain", "pa"), None))
    return jax.shard_map(shards, mesh=mesh, in_specs=in_specs, out_specs=out_specs, check_vma=False)
```

```python
import functools

import jax
import jax.numpy as jnp
import numpy as np
from jax import lax
from jax.experimental import pallas as pl
from jax.experimental.pallas import tpu as pltpu
from jax.sharding import PartitionSpec as P

MESH = pl.DeviceIdType.MESH
STEPS = 5
SUB = 8

diffuse_cross = 0.15
diffuse_along = 16.0

ZLO, ZHI, YLO, YHI = range(4)
CZP, CZM, CYP, CYM, CXP, CXM, SRC, OBS = range(8)


def implicit_matrix(length):
    banded = (1.0 + 2.0 * diffuse_along) * np.eye(length) - diffuse_along * (
        np.eye(length, k=1) + np.eye(length, k=-1)
    )
    matrix = np.linalg.inv(banded).astype(np.float32)
    high = matrix.astype(jnp.bfloat16)
    low = (matrix - high.astype(np.float32)).astype(jnp.bfloat16)
    return jnp.asarray(high), jnp.asarray(low)


def kernel(
    *refs,
):
    inputs, (hessian_ref, gram_ref), refs = refs[:8], refs[8:10], refs[10:]
    loaded, refs = refs[:8], refs[8:]
    probes_ref, vel_ref, prior_ref, noise_ref, smask_ref, omask_ref, mhi_ref, mlo_ref = loaded
    (
    u_ref,
    s_ref,
    b_ref,
    coef_ref,
    whi_ref,
    wlo_ref,
    zh_ref,
    yh_ref,
    zs_ref,
    ys_ref,
    send_sem,
    recv_sem,
    load_sem,
    out_ref,
    out_sem,
    pu_ref,
    acc_ref,
    sum_ref,
    gt_ref,
    gr_ref,
    pair_send,
    pair_recv,
    ys_sem,
    yr_sem,
    zs_sem,
    zr_sem,
    core_sem,
    word_sem,
    ytile_ref,
    ztile_ref,
    ) = refs
    count, nz, ny, nx = probes_ref.shape
    tiles = ny // SUB
    zi, yi = lax.axis_index("gz"), lax.axis_index("gy")
    zn, yn = lax.axis_size("gz"), lax.axis_size("gy")
    exists = [zi > 0, zi < zn - 1, yi > 0, yi < yn - 1]
    target = [
        {"gz": lax.max(zi - 1, 0)},
        {"gz": lax.min(zi + 1, zn - 1)},
        {"gy": lax.max(yi - 1, 0)},
        {"gy": lax.min(yi + 1, yn - 1)},
    ]

    own = lax.axis_index("pa")
    half = nz // 2

    def crossed(me, distance):
        return me + distance * (1 - 2 * ((me // distance) % 2))

    def doubled(axis, me, n):
        return [{axis: crossed(me, 1 << k)} for k in range((n - 1).bit_length())]

    other_core = {"pa": 1 - own}
    y_doubled, z_doubled = doubled("gy", yi, yn), doubled("gz", zi, zn)
    z_other = zi - 1 + 2 * (zi % 2)
    y_other = yi - 1 + 2 * (yi % 2)
    met = [
        ((z_other >= 0) & (z_other < zn), {"gz": lax.clamp(0, z_other, zn - 1)}),
        ((y_other >= 0) & (y_other < yn), {"gy": lax.clamp(0, y_other, yn - 1)}),
    ]

    probe_loads = [
        pltpu.make_async_copy(inputs[0].at[p], probes_ref.at[p], load_sem.at[8 + p]) for p in range(count)
    ]
    loads = [None] + [pltpu.make_async_copy(inputs[k], loaded[k], load_sem.at[k]) for k in range(1, 8)]
    for copy in (loads[2], loads[4], probe_loads[0], loads[6], loads[7], *probe_loads[1:]):
        copy.start()
    for copy in (loads[1], loads[3], loads[5]):
        copy.start()

    barrier = pltpu.get_barrier_semaphore()
    greeted = [other_core] + y_doubled + z_doubled[:3]
    for device in greeted:
        pl.semaphore_signal(barrier, inc=1, device_id=device, device_id_type=MESH)
    for there, device in met:

        @pl.when(there)
        def _():
            pl.semaphore_signal(barrier, inc=1, device_id=device, device_id_type=MESH)

    row = lax.broadcasted_iota(jnp.int32, (SUB, nx), 0)
    first_row, last_row = row == 0, row == SUB - 1
    lane = lax.broadcasted_iota(jnp.int32, (ny, nx), 1)

    def prepare(z, _):
        vx, vy, vz = (0.5 * vel_ref[c, z] for c in range(3))
        coef_ref[CZP, z] = diffuse_cross - vz
        coef_ref[CZM, z] = diffuse_cross + vz
        coef_ref[CYP, z] = diffuse_cross - vy
        coef_ref[CYM, z] = diffuse_cross + vy
        coef_ref[CXP, z] = jnp.where(lane == nx - 1, 0.0, -vx)
        coef_ref[CXM, z] = jnp.where(lane == 0, 0.0, vx)
        coef_ref[OBS, z] = omask_ref[z].astype(jnp.float32) * noise_ref[z]
        return 0

    @pl.when(zi == 0)
    def _():
        zh_ref[:, 0] = jnp.zeros(zh_ref.shape[:1] + zh_ref.shape[2:], jnp.float32)

    @pl.when(zi == zn - 1)
    def _():
        zh_ref[:, 1] = jnp.zeros(zh_ref.shape[:1] + zh_ref.shape[2:], jnp.float32)

    @pl.when(yi == 0)
    def _():
        yh_ref[:, 0] = jnp.zeros(yh_ref.shape[:1] + yh_ref.shape[2:], jnp.float32)

    @pl.when(yi == yn - 1)
    def _():
        yh_ref[:, 1] = jnp.zeros(yh_ref.shape[:1] + yh_ref.shape[2:], jnp.float32)

    acc_ref[...] = jnp.zeros(acc_ref.shape, jnp.float32)
    loads[2].wait()
    loads[4].wait()
    coef_ref[SRC] = smask_ref[...].astype(jnp.float32) * prior_ref[...]
    loads[6].wait()
    loads[7].wait()
    pl.semaphore_wait(barrier, len(greeted) + sum(there.astype(jnp.int32) for there, _ in met))

    def copies(slot, q, sources):
        result = []
        for side in range(4):
            halo = zh_ref if side < 2 else yh_ref
            result.append(
                pltpu.make_async_remote_copy(
                    src_ref=sources[side],
                    dst_ref=halo.at[slot, (side % 2) ^ 1, pl.ds(2 * q, 2)],
                    send_sem=send_sem.at[slot, side, q],
                    recv_sem=recv_sem.at[slot, side ^ 1, q],
                    device_id=target[side],
                    device_id_type=MESH,
                )
            )
        return result

    def send(slot, q, sources):
        for side, copy in enumerate(copies(slot, q, sources)):
            pl.when(exists[side])(copy.start)

    def settle(slot, q, sources):
        moved = copies(slot, q, sources)
        for side in range(4):

            @pl.when(exists[side])
            def _():
                moved[side ^ 1].wait_recv()
                moved[side].wait_send()

    def state_sources(n, slot, q):
        two = pl.ds(2 * q, 2)
        return [u_ref.at[n, two, 0], u_ref.at[n, two, nz - 1], ys_ref.at[slot, 0, two], ys_ref.at[slot, 1, two]]

    def adjoint_sources(slot, q):
        return [source.at[slot, side, pl.ds(2 * q, 2)] for source in (zs_ref, ys_ref) for side in range(2)]

    def both(q, *parts):
        for part in parts:
            for r in range(2):
                part(r, 2 * q + r)

    def put(r, z, pair, left, right):
        rows = jnp.concatenate([left, right], axis=0)
        high = rows.astype(jnp.bfloat16)
        low = (rows - high.astype(jnp.float32)).astype(jnp.bfloat16)
        where = pl.ds(z * ny + pair * 2 * SUB, 2 * SUB)
        whi_ref[r, where, :] = high
        wlo_ref[r, where, :] = low

    def solve(r):
        dot = functools.partial(jnp.dot, preferred_element_type=jnp.float32)
        high, low = whi_ref[r], wlo_ref[r]
        moved = dot(high, mhi_ref[...]) + (dot(high, mlo_ref[...]) + dot(low, mhi_ref[...]))
        return moved.reshape(nz, ny, nx)

    def by_tile(r, make):
        for z in range(nz):
            for pair in range(tiles // 2):
                put(r, z, pair, make(z, 2 * pair), make(z, 2 * pair + 1))

    def rows_of(t):
        return pl.ds(t * SUB, SUB)

    def coef(kind, z, t):
        return coef_ref[kind, z, rows_of(t), :]

    def forward(r, n, slot, p):
        def make(z, t):
            def at(zz, tt):
                return u_ref[n, p, zz, rows_of(tt), :]

            centre = at(z, t)
            plus_z = at(z + 1, t) if z < nz - 1 else zh_ref[slot, 1, p, rows_of(t), :]
            minus_z = at(z - 1, t) if z > 0 else zh_ref[slot, 0, p, rows_of(t), :]
            if t < tiles - 1:
                above = pltpu.roll(at(z, t + 1), SUB - 1, 0)
            else:
                above = jnp.broadcast_to(yh_ref[slot, 1, p, pl.ds(z, 1), :], (SUB, nx))
            if t > 0:
                below = pltpu.roll(at(z, t - 1), 1, 0)
            else:
                below = jnp.broadcast_to(yh_ref[slot, 0, p, pl.ds(z, 1), :], (SUB, nx))
            plus_y = jnp.where(last_row, above, pltpu.roll(centre, SUB - 1, 0))
            minus_y = jnp.where(first_row, below, pltpu.roll(centre, 1, 0))
            total = (1.0 - 4.0 * diffuse_cross) * centre + s_ref[p, z, rows_of(t), :]
            total = total + (coef(CZP, z, t) * plus_z + coef(CZM, z, t) * minus_z)
            total = total + (coef(CYP, z, t) * plus_y + coef(CYM, z, t) * minus_y)
            return total + (
                coef(CXP, z, t) * pltpu.roll(centre, nx - 1, 1) + coef(CXM, z, t) * pltpu.roll(centre, 1, 1)
            )

        by_tile(r, make)

    def backward(r, n, slot, p):
        def make(z, t):
            def at(zz, tt):
                return b_ref[p, zz, rows_of(tt), :]

            centre = at(z, t)
            if z < nz - 1:
                plus_z = coef(CZM, z + 1, t) * at(z + 1, t)
            else:
                plus_z = zh_ref[slot, 1, p, rows_of(t), :]
            if z > 0:
                minus_z = coef(CZP, z - 1, t) * at(z - 1, t)
            else:
                minus_z = zh_ref[slot, 0, p, rows_of(t), :]
            if t < tiles - 1:
                above = pltpu.roll(coef(CYM, z, t + 1) * at(z, t + 1), SUB - 1, 0)
            else:
                above = jnp.broadcast_to(yh_ref[slot, 1, p, pl.ds(z, 1), :], (SUB, nx))
            if t > 0:
                below = pltpu.roll(coef(CYP, z, t - 1) * at(z, t - 1), 1, 0)
            else:
                below = jnp.broadcast_to(yh_ref[slot, 0, p, pl.ds(z, 1), :], (SUB, nx))
            plus_y = jnp.where(last_row, above, pltpu.roll(coef(CYM, z, t) * centre, SUB - 1, 0))
            minus_y = jnp.where(first_row, below, pltpu.roll(coef(CYP, z, t) * centre, 1, 0))
            total = (1.0 - 4.0 * diffuse_cross) * centre + coef(OBS, z, t) * u_ref[n, p, z, rows_of(t), :]
            total = total + (plus_z + minus_z)
            total = total + (plus_y + minus_y)
            return total + (
                pltpu.roll(coef(CXM, z, t) * centre, nx - 1, 1) + pltpu.roll(coef(CXP, z, t) * centre, 1, 1)
            )

        by_tile(r, make)

    def finish_state(r, n, slot, p):
        state = solve(r)
        u_ref[n, p] = state
        for z in range(nz):
            ys_ref[slot, 0, p, pl.ds(z, 1), :] = state[z, 0:1, :]
            ys_ref[slot, 1, p, pl.ds(z, 1), :] = state[z, ny - 1 : ny, :]

    def finish_adjoint(slot, p, pulled):
        b_ref[p] = pulled
        zs_ref[slot, 0, p] = coef_ref[CZM, 0] * pulled[0]
        zs_ref[slot, 1, p] = coef_ref[CZP, nz - 1] * pulled[nz - 1]
        for z in range(nz):
            ys_ref[slot, 0, p, pl.ds(z, 1), :] = coef_ref[CYM, z, 0:1, :] * pulled[z, 0:1, :]
            ys_ref[slot, 1, p, pl.ds(z, 1), :] = coef_ref[CYP, z, ny - 1 : ny, :] * pulled[z, ny - 1 : ny, :]

    def pair_copy(n):
        return pltpu.make_async_remote_copy(
            src_ref=u_ref.at[n, :, pl.ds((1 - own) * half, half)],
            dst_ref=pu_ref.at[n],
            send_sem=pair_send.at[n],
            recv_sem=pair_recv.at[n],
            device_id=other_core,
            device_id_type=MESH,
        )

    def core_tile():
        return pltpu.make_async_remote_copy(
            src_ref=gt_ref.at[0],
            dst_ref=gr_ref,
            send_sem=core_sem.at[0],
            recv_sem=core_sem.at[1],
            device_id=other_core,
            device_id_type=MESH,
        )

    def along(axis, me, n, tiles_ref, source, out_sem, in_sem):
        def move(distance):
            return pltpu.make_async_remote_copy(
                src_ref=source,
                dst_ref=tiles_ref.at[me],
                send_sem=out_sem.at[distance],
                recv_sem=in_sem.at[me],
                device_id={axis: (me + distance) % n},
                device_id_type=MESH,
            )

        def arrival(who):
            return pltpu.make_async_remote_copy(
                src_ref=source,
                dst_ref=tiles_ref.at[who],
                send_sem=out_sem.at[0],
                recv_sem=in_sem.at[who],
                device_id={axis: (me + 1) % n},
                device_id_type=MESH,
            )

        def start():
            def step(distance, _):
                move(distance).start()
                return 0

            lax.fori_loop(1, n, step, 0)

        def end():
            def step(distance, _):
                arrival((me + distance) % n).wait_recv()
                move(distance).wait_send()
                return 0

            lax.fori_loop(1, n, step, 0)
            tiles_ref[me] = source[...]
            total = tiles_ref[0]
            for who in range(1, n):
                total = total + tiles_ref[who]
            return total

        return start, end

    start_y, end_y = along("gy", yi, yn, ytile_ref, gt_ref.at[2], ys_sem, yr_sem)
    start_z, end_z = along("gz", zi, zn, ztile_ref, gt_ref.at[3], zs_sem, zr_sem)

    def pass_word(k):
        if 0 < k <= len(z_doubled[:3]):
            pl.semaphore_wait(word_sem.at[k - 1], 1)
        if k < len(z_doubled[:3]):
            pl.semaphore_signal(word_sem.at[k], inc=1, device_id=z_doubled[k], device_id_type=MESH)

    near = count // 2 + 1
    lanes = 128
    pieces = [(t, h) for t in range(tiles) for h in range(nx // lanes)]

    def gram_unit(n, i):
        if count != 8:
            raise NotImplementedError
        wait_pair = pl.when(i == 0)

        @wait_pair
        def _():
            pair_copy(n).wait()

        def own_terms(k, sums):
            sums = list(sums)
            for z in (2 * k, 2 * k + 1):
                for t, h in pieces:
                    where = (rows_of(t), pl.ds(h * lanes, lanes))
                    x = [u_ref[(n, (i + d) % count, z) + where] for d in range(near + 1)]
                    weight = coef_ref[(OBS, z) + where]
                    for r in range(2):
                        scaled = weight * x[r]
                        for d in range(near):
                            sums[r * near + d] = sums[r * near + d] + scaled * x[r + d]
            return tuple(sums)

        def pair_terms(k, sums):
            sums = list(sums)
            for z in (2 * k, 2 * k + 1):
                for t, h in pieces:
                    where = (rows_of(t), pl.ds(h * lanes, lanes))
                    weight = coef_ref[(OBS, own * half + z) + where]
                    scaled = [weight * u_ref[(n, i + r, own * half + z) + where] for r in range(2)]
                    for j in range(count):
                        y = pu_ref[(n, j, z) + where]
                        for r in range(2):
                            sums[r * count + j] = sums[r * count + j] + scaled[r] * y
            return tuple(sums)

        zero = jnp.zeros((SUB, lanes), jnp.float32)
        sums = lax.fori_loop(0, nz // 2, own_terms, (zero,) * (2 * near))
        for r in range(2):
            for d in range(near):
                acc_ref[i + r, d] += sums[r * near + d]
        sums = lax.fori_loop(0, half // 2, pair_terms, (zero,) * (2 * count))
        for r in range(2):
            for j in range(count):
                acc_ref[i + r, near + j] += sums[r * count + j]

    def gram_tile():
        ones = jnp.ones((lanes, lanes), jnp.float32)
        kinds = near + count

        def by_lanes(i, _):
            partial = acc_ref[i].reshape(kinds * SUB, lanes)
            total = jnp.dot(
                partial, ones, precision=lax.Precision.HIGHEST, preferred_element_type=jnp.float32
            )
            sum_ref[i] = total.reshape(kinds, SUB, lanes)
            return 0

        lax.fori_loop(0, count, by_lanes, 0)
        at_row = lax.broadcasted_iota(jnp.int32, (SUB, lanes), 0)
        at_lane = lax.broadcasted_iota(jnp.int32, (SUB, lanes), 1)
        mine, theirs = at_lane - own * count, at_lane - (1 - own) * count
        tile = jnp.zeros((SUB, lanes), jnp.float32)
        sent = jnp.zeros((SUB, lanes), jnp.float32)
        for i in range(count):
            for k in range(kinds):
                value = sum_ref[i, k]
                for shift in (4, 2, 1):
                    value = value + pltpu.roll(value, shift, 0)
                if k < near:
                    j = (i + k) % count
                    here = (at_row == i) & (mine == j)
                    if 0 < k < near - 1:
                        here = here | ((at_row == j) & (mine == i))
                    tile = tile + jnp.where(here, value, 0.0)
                else:
                    j = k - near
                    tile = tile + jnp.where((at_row == i) & (theirs == j), value, 0.0)
                    sent = sent + jnp.where((at_row == j) & (mine == i), value, 0.0)
        gt_ref[0] = sent
        gt_ref[1] = tile

    def end_core():
        core_tile().wait()
        gt_ref[2] = gt_ref[1] + gr_ref[...]
        start_y()

    def end_rows():
        gt_ref[3] = end_y()
        start_z()

    def out_copy(p):
        return pltpu.make_async_copy(out_ref.at[p], hessian_ref.at[p], out_sem.at[p])

    last = STEPS - 1

    pairs = count // 2

    def first_step(q, _):
        def source(r, p):
            pltpu.make_async_copy(inputs[0].at[p], probes_ref.at[p], load_sem.at[8 + p]).wait()
            for z in range(nz):
                for t in range(tiles):
                    s_ref[p, z, rows_of(t), :] = coef(SRC, z, t) * probes_ref[p, z, rows_of(t), :]
            by_tile(r, lambda z, t: coef(SRC, z, t) * probes_ref[p, z, rows_of(t), :])

        both(q, source, lambda r, p: finish_state(r, 0, 0, p))
        send(0, q, state_sources(0, 0, q))
        return 0

    lax.fori_loop(0, pairs, first_step, 0)
    pair_copy(0).start()
    for k in (1, 3, 5):
        loads[k].wait()
    lax.fori_loop(0, nz, prepare, 0)

    def forward_step(i, _):
        n, q = i // pairs + 1, i % pairs
        before, now = (n + 1) % 2, n % 2
        settle(before, q, state_sources(n - 1, before, q))
        both(
            q,
            lambda r, p: forward(r, n - 1, before, p),
            lambda r, p: finish_state(r, n, now, p),
        )
        send(now, q, state_sources(n, now, q))

        @pl.when(q == pairs - 1)
        def _():
            pair_copy(n).start()

        gram_unit(n - 1, 2 * q)
        return 0

    lax.fori_loop(0, (last - 1) * pairs, forward_step, 0)

    def turn_step(q, _):
        before, now = (last + 1) % 2, last % 2
        settle(before, q, state_sources(last - 1, before, q))

        def turn(r, p):
            u_ref[last, p] = solve(r)
            by_tile(r, lambda z, t: coef(OBS, z, t) * u_ref[last, p, z, rows_of(t), :])

        def pull(r, p):
            pulled = solve(r)
            out_ref[p] = pulled
            finish_adjoint(now, p, pulled)

        both(q, lambda r, p: forward(r, last - 1, before, p), turn, pull)
        send(now, q, adjoint_sources(now, q))
        gram_unit(last - 1, 2 * q)
        return 0

    lax.fori_loop(0, pairs, turn_step, 0)
    pair_copy(last).start()
    pass_word(0)

    def backward_step(i, _):
        k, q = i // pairs + 1, i % pairs
        before, now = (last + k + 1) % 2, (last + k) % 2
        settle(before, q, adjoint_sources(before, q))

        def pull(r, p):
            pulled = solve(r)
            out_ref[p] += pulled
            finish_adjoint(now, p, pulled)

        both(q, lambda r, p: backward(r, last - k, before, p), pull)
        send(now, q, adjoint_sources(now, q))

        for turn, when in enumerate((0, 2, 4)):

            @pl.when(i == when)
            def _():
                pass_word(turn + 1)

        @pl.when((i >= 1) & (i < 3))
        def _():
            def unit(r, _):
                gram_unit(last, 4 * (i - 1) + 2 * r)
                return 0

            lax.fori_loop(0, 2, unit, 0)

        @pl.when(i == 2)
        def _():
            gram_tile()
            core_tile().start()

        pl.when(i == 3)(end_core)
        pl.when(i == 5)(end_rows)
        return 0

    lax.fori_loop(0, (last - 1) * pairs, backward_step, 0)

    def last_step(q, _):
        before = (2 * last + 1) % 2
        settle(before, q, adjoint_sources(before, q))

        def pull(r, p):
            out_ref[p] = coef_ref[SRC] * (out_ref[p] + solve(r))

        both(q, lambda r, p: backward(r, 0, before, p), pull, lambda r, p: out_copy(p).start())
        return 0

    lax.fori_loop(0, pairs, last_step, 0)
    for p in range(count):
        out_copy(p).wait()
    gram_ref[...] = end_z()[:, : gram_ref.shape[1]] / (nz * ny * nx * zn * yn)


def shards(probes, velocity, prior_scale, noise_precision, source_mask, sensor_mask):
    count, nz, ny, nx = probes.shape
    high, low = implicit_matrix(nx)
    arguments = (probes, velocity, prior_scale, noise_precision, source_mask, sensor_mask, high, low)
    cores = lax.axis_size("pa")
    zn, yn = lax.axis_size("gz"), lax.axis_size("gy")
    near = count // 2 + 1
    return pl.pallas_call(
        kernel,
        out_shape=(
            jax.ShapeDtypeStruct(probes.shape, jnp.float32),
            jax.ShapeDtypeStruct((count, cores * count), jnp.float32),
        ),
        in_specs=[pl.BlockSpec(memory_space=pltpu.HBM)] * len(arguments),
        out_specs=(pl.BlockSpec(memory_space=pltpu.HBM), pl.BlockSpec(memory_space=pltpu.VMEM)),
        scratch_shapes=[
            *(pltpu.VMEM(array.shape, array.dtype) for array in arguments),
            pltpu.VMEM((STEPS, count, nz, ny, nx), jnp.float32),
            pltpu.VMEM((count, nz, ny, nx), jnp.float32),
            pltpu.VMEM((count, nz, ny, nx), jnp.float32),
            pltpu.VMEM((8, nz, ny, nx), jnp.float32),
            pltpu.VMEM((2, nz * ny, nx), jnp.bfloat16),
            pltpu.VMEM((2, nz * ny, nx), jnp.bfloat16),
            pltpu.VMEM((2, 2, count, ny, nx), jnp.float32),
            pltpu.VMEM((2, 2, count, nz, nx), jnp.float32),
            pltpu.VMEM((2, 2, count, ny, nx), jnp.float32),
            pltpu.VMEM((2, 2, count, nz, nx), jnp.float32),
            pltpu.SemaphoreType.DMA((2, 4, count // 2)),
            pltpu.SemaphoreType.DMA((2, 4, count // 2)),
            pltpu.SemaphoreType.DMA((8 + count,)),
            pltpu.VMEM((count, nz, ny, nx), jnp.float32),
            pltpu.SemaphoreType.DMA((count,)),
            pltpu.VMEM((STEPS, count, nz // 2, ny, nx), jnp.float32),
            pltpu.VMEM((count, near + count, SUB, 128), jnp.float32),
            pltpu.VMEM((count, near + count, SUB, 128), jnp.float32),
            pltpu.VMEM((4, SUB, 128), jnp.float32),
            pltpu.VMEM((SUB, 128), jnp.float32),
            pltpu.SemaphoreType.DMA((STEPS,)),
            pltpu.SemaphoreType.DMA((STEPS,)),
            pltpu.SemaphoreType.DMA((yn,)),
            pltpu.SemaphoreType.DMA((yn,)),
            pltpu.SemaphoreType.DMA((zn,)),
            pltpu.SemaphoreType.DMA((zn,)),
            pltpu.SemaphoreType.DMA((2,)),
            pltpu.SemaphoreType.REGULAR((3,)),
            pltpu.VMEM((yn, SUB, 128), jnp.float32),
            pltpu.VMEM((zn, SUB, 128), jnp.float32),
        ],
        compiler_params=pltpu.CompilerParams(
            collective_id=0, has_side_effects=True, vmem_limit_bytes=60 * 1024 * 1024
        ),
        name="solve",
    )(*arguments)


def solution(mesh):
    in_specs = (
        P(("chain", "pa"), "gz", "gy", None),
        P(None, ("chain", "gz"), "gy", None),
        P(("chain", "gz"), "gy", None),
        P(("chain", "gz"), "gy", None),
        P(("chain", "gz"), "gy", None),
        P(("chain", "gz"), "gy", None),
    )
    out_specs = (P(("chain", "pa"), "gz", "gy", None), P(("chain", "pa"), None))
    return jax.shard_map(shards, mesh=mesh, in_specs=in_specs, out_specs=out_specs, check_vma=False)
```

```python
import functools

import jax
import jax.numpy as jnp
import numpy as np
from jax import lax
from jax.experimental import pallas as pl
from jax.experimental.pallas import tpu as pltpu
from jax.sharding import PartitionSpec as P

MESH = pl.DeviceIdType.MESH
STEPS = 5
SUB = 8

diffuse_cross = 0.15
diffuse_along = 16.0

ZLO, ZHI, YLO, YHI = range(4)
CZP, CZM, CYP, CYM, CXP, CXM, SRC, OBS = range(8)


def implicit_matrix(length):
    banded = (1.0 + 2.0 * diffuse_along) * np.eye(length) - diffuse_along * (
        np.eye(length, k=1) + np.eye(length, k=-1)
    )
    matrix = np.linalg.inv(banded).astype(np.float32)
    high = matrix.astype(jnp.bfloat16)
    low = (matrix - high.astype(np.float32)).astype(jnp.bfloat16)
    return jnp.asarray(high), jnp.asarray(low)


def kernel(
    *refs,
):
    inputs, (hessian_ref, gram_ref), refs = refs[:8], refs[8:10], refs[10:]
    loaded, refs = refs[:8], refs[8:]
    probes_ref, vel_ref, prior_ref, noise_ref, smask_ref, omask_ref, mhi_ref, mlo_ref = loaded
    (
    u_ref,
    s_ref,
    b_ref,
    coef_ref,
    whi_ref,
    wlo_ref,
    zh_ref,
    yh_ref,
    zs_ref,
    ys_ref,
    send_sem,
    recv_sem,
    load_sem,
    out_ref,
    out_sem,
    pu_ref,
    acc_ref,
    sum_ref,
    gt_ref,
    gr_ref,
    pair_send,
    pair_recv,
    ys_sem,
    yr_sem,
    zs_sem,
    zr_sem,
    core_sem,
    word_sem,
    ytile_ref,
    ztile_ref,
    ) = refs
    count, nz, ny, nx = probes_ref.shape
    tiles = ny // SUB
    zi, yi = lax.axis_index("gz"), lax.axis_index("gy")
    zn, yn = lax.axis_size("gz"), lax.axis_size("gy")
    exists = [zi > 0, zi < zn - 1, yi > 0, yi < yn - 1]
    target = [
        {"gz": lax.max(zi - 1, 0)},
        {"gz": lax.min(zi + 1, zn - 1)},
        {"gy": lax.max(yi - 1, 0)},
        {"gy": lax.min(yi + 1, yn - 1)},
    ]

    own = lax.axis_index("pa")
    half = nz // 2

    def crossed(me, distance):
        return me + distance * (1 - 2 * ((me // distance) % 2))

    def doubled(axis, me, n):
        return [{axis: crossed(me, 1 << k)} for k in range((n - 1).bit_length())]

    other_core = {"pa": 1 - own}
    y_doubled, z_doubled = doubled("gy", yi, yn), doubled("gz", zi, zn)
    z_other = zi - 1 + 2 * (zi % 2)
    y_other = yi - 1 + 2 * (yi % 2)
    met = [
        ((z_other >= 0) & (z_other < zn), {"gz": lax.clamp(0, z_other, zn - 1)}),
        ((y_other >= 0) & (y_other < yn), {"gy": lax.clamp(0, y_other, yn - 1)}),
    ]

    probe_loads = [
        pltpu.make_async_copy(inputs[0].at[p], probes_ref.at[p], load_sem.at[8 + p]) for p in range(count)
    ]
    loads = [None] + [pltpu.make_async_copy(inputs[k], loaded[k], load_sem.at[k]) for k in range(1, 8)]
    for copy in (loads[2], loads[4], probe_loads[0], loads[6], loads[7], *probe_loads[1:]):
        copy.start()
    for copy in (loads[1], loads[3], loads[5]):
        copy.start()

    barrier = pltpu.get_barrier_semaphore()
    greeted = [other_core] + y_doubled + z_doubled[:3]
    for device in greeted:
        pl.semaphore_signal(barrier, inc=1, device_id=device, device_id_type=MESH)
    for there, device in met:

        @pl.when(there)
        def _():
            pl.semaphore_signal(barrier, inc=1, device_id=device, device_id_type=MESH)

    row = lax.broadcasted_iota(jnp.int32, (SUB, nx), 0)
    first_row, last_row = row == 0, row == SUB - 1
    lane = lax.broadcasted_iota(jnp.int32, (ny, nx), 1)

    def prepare(z, _):
        vx, vy, vz = (0.5 * vel_ref[c, z] for c in range(3))
        coef_ref[CZP, z] = diffuse_cross - vz
        coef_ref[CZM, z] = diffuse_cross + vz
        coef_ref[CYP, z] = diffuse_cross - vy
        coef_ref[CYM, z] = diffuse_cross + vy
        coef_ref[CXP, z] = jnp.where(lane == nx - 1, 0.0, -vx)
        coef_ref[CXM, z] = jnp.where(lane == 0, 0.0, vx)
        coef_ref[OBS, z] = omask_ref[z].astype(jnp.float32) * noise_ref[z]
        return 0

    @pl.when(zi == 0)
    def _():
        zh_ref[:, 0] = jnp.zeros(zh_ref.shape[:1] + zh_ref.shape[2:], jnp.float32)

    @pl.when(zi == zn - 1)
    def _():
        zh_ref[:, 1] = jnp.zeros(zh_ref.shape[:1] + zh_ref.shape[2:], jnp.float32)

    @pl.when(yi == 0)
    def _():
        yh_ref[:, 0] = jnp.zeros(yh_ref.shape[:1] + yh_ref.shape[2:], jnp.float32)

    @pl.when(yi == yn - 1)
    def _():
        yh_ref[:, 1] = jnp.zeros(yh_ref.shape[:1] + yh_ref.shape[2:], jnp.float32)

    loads[2].wait()
    loads[4].wait()
    coef_ref[SRC] = smask_ref[...].astype(jnp.float32) * prior_ref[...]
    loads[6].wait()
    loads[7].wait()
    pl.semaphore_wait(barrier, len(greeted) + sum(there.astype(jnp.int32) for there, _ in met))

    def copies(slot, q, sources):
        result = []
        for side in range(4):
            halo = zh_ref if side < 2 else yh_ref
            result.append(
                pltpu.make_async_remote_copy(
                    src_ref=sources[side],
                    dst_ref=halo.at[slot, (side % 2) ^ 1, pl.ds(2 * q, 2)],
                    send_sem=send_sem.at[slot, side, q],
                    recv_sem=recv_sem.at[slot, side ^ 1, q],
                    device_id=target[side],
                    device_id_type=MESH,
                )
            )
        return result

    def send(slot, q, sources):
        for side, copy in enumerate(copies(slot, q, sources)):
            pl.when(exists[side])(copy.start)

    def settle(slot, q, sources):
        moved = copies(slot, q, sources)
        for side in range(4):

            @pl.when(exists[side])
            def _():
                moved[side ^ 1].wait_recv()
                moved[side].wait_send()

    def state_sources(n, slot, q):
        two = pl.ds(2 * q, 2)
        return [u_ref.at[n, two, 0], u_ref.at[n, two, nz - 1], ys_ref.at[slot, 0, two], ys_ref.at[slot, 1, two]]

    def adjoint_sources(slot, q):
        return [source.at[slot, side, pl.ds(2 * q, 2)] for source in (zs_ref, ys_ref) for side in range(2)]

    def both(q, *parts):
        for part in parts:
            for r in range(2):
                part(r, 2 * q + r)

    def put(r, z, pair, left, right):
        rows = jnp.concatenate([left, right], axis=0)
        high = rows.astype(jnp.bfloat16)
        low = (rows - high.astype(jnp.float32)).astype(jnp.bfloat16)
        where = pl.ds(z * ny + pair * 2 * SUB, 2 * SUB)
        whi_ref[r, where, :] = high
        wlo_ref[r, where, :] = low

    def solve(r):
        dot = functools.partial(jnp.dot, preferred_element_type=jnp.float32)
        high, low = whi_ref[r], wlo_ref[r]
        moved = dot(high, mhi_ref[...]) + (dot(high, mlo_ref[...]) + dot(low, mhi_ref[...]))
        return moved.reshape(nz, ny, nx)

    def by_tile(r, make):
        for z in range(nz):
            for pair in range(tiles // 2):
                put(r, z, pair, make(z, 2 * pair), make(z, 2 * pair + 1))

    def rows_of(t):
        return pl.ds(t * SUB, SUB)

    def coef(kind, z, t):
        return coef_ref[kind, z, rows_of(t), :]

    def forward(r, n, slot, p):
        def make(z, t):
            def at(zz, tt):
                return u_ref[n, p, zz, rows_of(tt), :]

            centre = at(z, t)
            plus_z = at(z + 1, t) if z < nz - 1 else zh_ref[slot, 1, p, rows_of(t), :]
            minus_z = at(z - 1, t) if z > 0 else zh_ref[slot, 0, p, rows_of(t), :]
            if t < tiles - 1:
                above = pltpu.roll(at(z, t + 1), SUB - 1, 0)
            else:
                above = jnp.broadcast_to(yh_ref[slot, 1, p, pl.ds(z, 1), :], (SUB, nx))
            if t > 0:
                below = pltpu.roll(at(z, t - 1), 1, 0)
            else:
                below = jnp.broadcast_to(yh_ref[slot, 0, p, pl.ds(z, 1), :], (SUB, nx))
            plus_y = jnp.where(last_row, above, pltpu.roll(centre, SUB - 1, 0))
            minus_y = jnp.where(first_row, below, pltpu.roll(centre, 1, 0))
            total = (1.0 - 4.0 * diffuse_cross) * centre + s_ref[p, z, rows_of(t), :]
            total = total + (coef(CZP, z, t) * plus_z + coef(CZM, z, t) * minus_z)
            total = total + (coef(CYP, z, t) * plus_y + coef(CYM, z, t) * minus_y)
            return total + (
                coef(CXP, z, t) * pltpu.roll(centre, nx - 1, 1) + coef(CXM, z, t) * pltpu.roll(centre, 1, 1)
            )

        by_tile(r, make)

    def backward(r, n, slot, p):
        def make(z, t):
            def at(zz, tt):
                return b_ref[p, zz, rows_of(tt), :]

            centre = at(z, t)
            if z < nz - 1:
                plus_z = coef(CZM, z + 1, t) * at(z + 1, t)
            else:
                plus_z = zh_ref[slot, 1, p, rows_of(t), :]
            if z > 0:
                minus_z = coef(CZP, z - 1, t) * at(z - 1, t)
            else:
                minus_z = zh_ref[slot, 0, p, rows_of(t), :]
            if t < tiles - 1:
                above = pltpu.roll(coef(CYM, z, t + 1) * at(z, t + 1), SUB - 1, 0)
            else:
                above = jnp.broadcast_to(yh_ref[slot, 1, p, pl.ds(z, 1), :], (SUB, nx))
            if t > 0:
                below = pltpu.roll(coef(CYP, z, t - 1) * at(z, t - 1), 1, 0)
            else:
                below = jnp.broadcast_to(yh_ref[slot, 0, p, pl.ds(z, 1), :], (SUB, nx))
            plus_y = jnp.where(last_row, above, pltpu.roll(coef(CYM, z, t) * centre, SUB - 1, 0))
            minus_y = jnp.where(first_row, below, pltpu.roll(coef(CYP, z, t) * centre, 1, 0))
            total = (1.0 - 4.0 * diffuse_cross) * centre + coef(OBS, z, t) * u_ref[n, p, z, rows_of(t), :]
            total = total + (plus_z + minus_z)
            total = total + (plus_y + minus_y)
            return total + (
                pltpu.roll(coef(CXM, z, t) * centre, nx - 1, 1) + pltpu.roll(coef(CXP, z, t) * centre, 1, 1)
            )

        by_tile(r, make)

    def finish_state(r, n, slot, p):
        state = solve(r)
        u_ref[n, p] = state
        for z in range(nz):
            ys_ref[slot, 0, p, pl.ds(z, 1), :] = state[z, 0:1, :]
            ys_ref[slot, 1, p, pl.ds(z, 1), :] = state[z, ny - 1 : ny, :]

    def finish_adjoint(slot, p, pulled):
        b_ref[p] = pulled
        zs_ref[slot, 0, p] = coef_ref[CZM, 0] * pulled[0]
        zs_ref[slot, 1, p] = coef_ref[CZP, nz - 1] * pulled[nz - 1]
        for z in range(nz):
            ys_ref[slot, 0, p, pl.ds(z, 1), :] = coef_ref[CYM, z, 0:1, :] * pulled[z, 0:1, :]
            ys_ref[slot, 1, p, pl.ds(z, 1), :] = coef_ref[CYP, z, ny - 1 : ny, :] * pulled[z, ny - 1 : ny, :]

    def pair_copy(n):
        return pltpu.make_async_remote_copy(
            src_ref=u_ref.at[n, :, pl.ds((1 - own) * half, half)],
            dst_ref=pu_ref.at[n],
            send_sem=pair_send.at[n],
            recv_sem=pair_recv.at[n],
            device_id=other_core,
            device_id_type=MESH,
        )

    def core_tile():
        return pltpu.make_async_remote_copy(
            src_ref=gt_ref.at[0],
            dst_ref=gr_ref,
            send_sem=core_sem.at[0],
            recv_sem=core_sem.at[1],
            device_id=other_core,
            device_id_type=MESH,
        )

    def along(axis, me, n, tiles_ref, source, out_sem, in_sem):
        def move(distance):
            return pltpu.make_async_remote_copy(
                src_ref=source,
                dst_ref=tiles_ref.at[me],
                send_sem=out_sem.at[distance],
                recv_sem=in_sem.at[me],
                device_id={axis: (me + distance) % n},
                device_id_type=MESH,
            )

        def arrival(who):
            return pltpu.make_async_remote_copy(
                src_ref=source,
                dst_ref=tiles_ref.at[who],
                send_sem=out_sem.at[0],
                recv_sem=in_sem.at[who],
                device_id={axis: (me + 1) % n},
                device_id_type=MESH,
            )

        def start():
            def step(distance, _):
                move(distance).start()
                return 0

            lax.fori_loop(1, n, step, 0)

        def end():
            def step(distance, _):
                arrival((me + distance) % n).wait_recv()
                move(distance).wait_send()
                return 0

            lax.fori_loop(1, n, step, 0)
            tiles_ref[me] = source[...]
            total = tiles_ref[0]
            for who in range(1, n):
                total = total + tiles_ref[who]
            return total

        return start, end

    start_y, end_y = along("gy", yi, yn, ytile_ref, gt_ref.at[2], ys_sem, yr_sem)
    start_z, end_z = along("gz", zi, zn, ztile_ref, gt_ref.at[3], zs_sem, zr_sem)

    def pass_word(k):
        if 0 < k <= len(z_doubled[:3]):
            pl.semaphore_wait(word_sem.at[k - 1], 1)
        if k < len(z_doubled[:3]):
            pl.semaphore_signal(word_sem.at[k], inc=1, device_id=z_doubled[k], device_id_type=MESH)

    near = count // 2 + 1
    lanes = 128
    pieces = [(t, h) for t in range(tiles) for h in range(nx // lanes)]

    def gram_unit(n, i):
        if count != 8:
            raise NotImplementedError
        wait_pair = pl.when(i == 0)

        @wait_pair
        def _():
            pair_copy(n).wait()

        def own_terms(k, sums):
            sums = list(sums)
            for z in (2 * k, 2 * k + 1):
                for t, h in pieces:
                    where = (rows_of(t), pl.ds(h * lanes, lanes))
                    x = [u_ref[(n, (i + d) % count, z) + where] for d in range(near + 1)]
                    weight = coef_ref[(OBS, z) + where]
                    for r in range(2):
                        scaled = weight * x[r]
                        for d in range(near):
                            sums[r * near + d] = sums[r * near + d] + scaled * x[r + d]
            return tuple(sums)

        def pair_terms(k, sums):
            sums = list(sums)
            for z in (2 * k, 2 * k + 1):
                for t, h in pieces:
                    where = (rows_of(t), pl.ds(h * lanes, lanes))
                    weight = coef_ref[(OBS, own * half + z) + where]
                    scaled = [weight * u_ref[(n, i + r, own * half + z) + where] for r in range(2)]
                    for j in range(count):
                        y = pu_ref[(n, j, z) + where]
                        for r in range(2):
                            sums[r * count + j] = sums[r * count + j] + scaled[r] * y
            return tuple(sums)

        zero = jnp.zeros((SUB, lanes), jnp.float32)
        sums = lax.fori_loop(0, nz // 2, own_terms, (zero,) * (2 * near))
        for r in range(2):
            for d in range(near):
                acc_ref[i + r, d] += sums[r * near + d]
        sums = lax.fori_loop(0, half // 2, pair_terms, (zero,) * (2 * count))
        for r in range(2):
            for j in range(count):
                acc_ref[i + r, near + j] += sums[r * count + j]

    def gram_units(n, first, units):
        def unit(k, _):
            gram_unit(n, 2 * (first + k))
            return 0

        lax.fori_loop(0, units, unit, 0)

    def gram_tile():
        ones = jnp.ones((lanes, lanes), jnp.float32)
        kinds = near + count

        def by_lanes(i, _):
            partial = acc_ref[i].reshape(kinds * SUB, lanes)
            total = jnp.dot(
                partial, ones, precision=lax.Precision.HIGHEST, preferred_element_type=jnp.float32
            )
            sum_ref[i] = total.reshape(kinds, SUB, lanes)
            return 0

        lax.fori_loop(0, count, by_lanes, 0)
        at_row = lax.broadcasted_iota(jnp.int32, (SUB, lanes), 0)
        at_lane = lax.broadcasted_iota(jnp.int32, (SUB, lanes), 1)
        mine, theirs = at_lane - own * count, at_lane - (1 - own) * count
        tile = jnp.zeros((SUB, lanes), jnp.float32)
        sent = jnp.zeros((SUB, lanes), jnp.float32)
        for i in range(count):
            for k in range(kinds):
                value = sum_ref[i, k]
                for shift in (4, 2, 1):
                    value = value + pltpu.roll(value, shift, 0)
                if k < near:
                    j = (i + k) % count
                    here = (at_row == i) & (mine == j)
                    if 0 < k < near - 1:
                        here = here | ((at_row == j) & (mine == i))
                    tile = tile + jnp.where(here, value, 0.0)
                else:
                    j = k - near
                    tile = tile + jnp.where((at_row == i) & (theirs == j), value, 0.0)
                    sent = sent + jnp.where((at_row == j) & (mine == i), value, 0.0)
        gt_ref[0] = sent
        gt_ref[1] = tile

    def end_core():
        core_tile().wait()
        gt_ref[2] = gt_ref[1] + gr_ref[...]
        start_y()

    def end_rows():
        gt_ref[3] = end_y()
        start_z()

    def out_copy(p):
        return pltpu.make_async_copy(out_ref.at[p], hessian_ref.at[p], out_sem.at[p])

    last = STEPS - 1

    pairs = count // 2

    def first_step(q, _):
        def source(r, p):
            pltpu.make_async_copy(inputs[0].at[p], probes_ref.at[p], load_sem.at[8 + p]).wait()
            for z in range(nz):
                for t in range(tiles):
                    s_ref[p, z, rows_of(t), :] = coef(SRC, z, t) * probes_ref[p, z, rows_of(t), :]
            by_tile(r, lambda z, t: coef(SRC, z, t) * probes_ref[p, z, rows_of(t), :])

        both(q, source, lambda r, p: finish_state(r, 0, 0, p))
        send(0, q, state_sources(0, 0, q))
        return 0

    lax.fori_loop(0, pairs, first_step, 0)
    pair_copy(0).start()
    acc_ref[...] = jnp.zeros(acc_ref.shape, jnp.float32)
    for k in (1, 3, 5):
        loads[k].wait()
    lax.fori_loop(0, nz, prepare, 0)

    def forward_step(i, _):
        n, q = i // pairs + 1, i % pairs
        before, now = (n + 1) % 2, n % 2
        settle(before, q, state_sources(n - 1, before, q))
        both(
            q,
            lambda r, p: forward(r, n - 1, before, p),
            lambda r, p: finish_state(r, n, now, p),
        )
        send(now, q, state_sources(n, now, q))

        @pl.when(q == pairs - 1)
        def _():
            pair_copy(n).start()
            gram_units(n - 1, 0, pairs)

        return 0

    lax.fori_loop(0, (last - 1) * pairs, forward_step, 0)

    def turn_step(q, _):
        before, now = (last + 1) % 2, last % 2
        settle(before, q, state_sources(last - 1, before, q))

        def turn(r, p):
            u_ref[last, p] = solve(r)
            by_tile(r, lambda z, t: coef(OBS, z, t) * u_ref[last, p, z, rows_of(t), :])

        def pull(r, p):
            pulled = solve(r)
            out_ref[p] = pulled
            finish_adjoint(now, p, pulled)

        both(q, lambda r, p: forward(r, last - 1, before, p), turn, pull)
        send(now, q, adjoint_sources(now, q))
        return 0

    lax.fori_loop(0, pairs, turn_step, 0)
    pair_copy(last).start()
    pass_word(0)
    gram_units(last - 1, 0, pairs)

    def backward_step(i, _):
        k, q = i // pairs + 1, i % pairs
        before, now = (last + k + 1) % 2, (last + k) % 2
        settle(before, q, adjoint_sources(before, q))

        def pull(r, p):
            pulled = solve(r)
            out_ref[p] += pulled
            finish_adjoint(now, p, pulled)

        both(q, lambda r, p: backward(r, last - k, before, p), pull)
        send(now, q, adjoint_sources(now, q))

        for turn, when in enumerate((0, 2, 4)):

            @pl.when(i == when)
            def _():
                pass_word(turn + 1)

        @pl.when((i >= 1) & (i < 3))
        def _():
            gram_units(last, 2 * (i - 1), 2)

        @pl.when(i == 2)
        def _():
            gram_tile()
            core_tile().start()

        pl.when(i == 3)(end_core)
        pl.when(i == 5)(end_rows)
        return 0

    lax.fori_loop(0, (last - 1) * pairs, backward_step, 0)

    def last_step(q, _):
        before = (2 * last + 1) % 2
        settle(before, q, adjoint_sources(before, q))

        def pull(r, p):
            out_ref[p] = coef_ref[SRC] * (out_ref[p] + solve(r))

        both(q, lambda r, p: backward(r, 0, before, p), pull, lambda r, p: out_copy(p).start())
        return 0

    lax.fori_loop(0, pairs, last_step, 0)
    for p in range(count):
        out_copy(p).wait()
    gram_ref[...] = end_z()[:, : gram_ref.shape[1]] / (nz * ny * nx * zn * yn)


def hand_over(solved_ref, summed_ref, hessian_ref, gram_ref, probe_ref, tile_ref, sem):
    count = solved_ref.shape[0]
    moves = [(solved_ref.at[p], probe_ref.at[p], hessian_ref.at[p]) for p in range(count)]
    moves.append((summed_ref, tile_ref, gram_ref))
    takes = [pltpu.make_async_copy(a, b, sem.at[0, k]) for k, (a, b, _) in enumerate(moves)]
    gives = [pltpu.make_async_copy(b, c, sem.at[1, k]) for k, (_, b, c) in enumerate(moves)]
    for take in takes:
        take.start()
    for take, give in zip(takes, gives):
        take.wait()
        give.start()
    for give in gives:
        give.wait()


def shards(probes, velocity, prior_scale, noise_precision, source_mask, sensor_mask):
    count, nz, ny, nx = probes.shape
    high, low = implicit_matrix(nx)
    arguments = (probes, velocity, prior_scale, noise_precision, source_mask, sensor_mask, high, low)
    cores = lax.axis_size("pa")
    zn, yn = lax.axis_size("gz"), lax.axis_size("gy")
    near = count // 2 + 1
    solved, summed = pl.pallas_call(
        kernel,
        out_shape=(
            jax.ShapeDtypeStruct(probes.shape, jnp.float32),
            jax.ShapeDtypeStruct((count, cores * count), jnp.float32),
        ),
        in_specs=[pl.BlockSpec(memory_space=pltpu.HBM)] * len(arguments),
        out_specs=(pl.BlockSpec(memory_space=pltpu.HBM), pl.BlockSpec(memory_space=pltpu.VMEM)),
        scratch_shapes=[
            *(pltpu.VMEM(array.shape, array.dtype) for array in arguments),
            pltpu.VMEM((STEPS, count, nz, ny, nx), jnp.float32),
            pltpu.VMEM((count, nz, ny, nx), jnp.float32),
            pltpu.VMEM((count, nz, ny, nx), jnp.float32),
            pltpu.VMEM((8, nz, ny, nx), jnp.float32),
            pltpu.VMEM((2, nz * ny, nx), jnp.bfloat16),
            pltpu.VMEM((2, nz * ny, nx), jnp.bfloat16),
            pltpu.VMEM((2, 2, count, ny, nx), jnp.float32),
            pltpu.VMEM((2, 2, count, nz, nx), jnp.float32),
            pltpu.VMEM((2, 2, count, ny, nx), jnp.float32),
            pltpu.VMEM((2, 2, count, nz, nx), jnp.float32),
            pltpu.SemaphoreType.DMA((2, 4, count // 2)),
            pltpu.SemaphoreType.DMA((2, 4, count // 2)),
            pltpu.SemaphoreType.DMA((8 + count,)),
            pltpu.VMEM((count, nz, ny, nx), jnp.float32),
            pltpu.SemaphoreType.DMA((count,)),
            pltpu.VMEM((STEPS, count, nz // 2, ny, nx), jnp.float32),
            pltpu.VMEM((count, near + count, SUB, 128), jnp.float32),
            pltpu.VMEM((count, near + count, SUB, 128), jnp.float32),
            pltpu.VMEM((4, SUB, 128), jnp.float32),
            pltpu.VMEM((SUB, 128), jnp.float32),
            pltpu.SemaphoreType.DMA((STEPS,)),
            pltpu.SemaphoreType.DMA((STEPS,)),
            pltpu.SemaphoreType.DMA((yn,)),
            pltpu.SemaphoreType.DMA((yn,)),
            pltpu.SemaphoreType.DMA((zn,)),
            pltpu.SemaphoreType.DMA((zn,)),
            pltpu.SemaphoreType.DMA((2,)),
            pltpu.SemaphoreType.REGULAR((3,)),
            pltpu.VMEM((yn, SUB, 128), jnp.float32),
            pltpu.VMEM((zn, SUB, 128), jnp.float32),
        ],
        compiler_params=pltpu.CompilerParams(
            collective_id=0, has_side_effects=True, vmem_limit_bytes=60 * 1024 * 1024
        ),
        name="solve",
    )(*arguments)
    return pl.pallas_call(
        hand_over,
        out_shape=(
            jax.ShapeDtypeStruct(probes.shape, jnp.float32),
            jax.ShapeDtypeStruct((count, cores * count), jnp.float32),
        ),
        in_specs=[pl.BlockSpec(memory_space=pltpu.HBM)] * 2,
        out_specs=(pl.BlockSpec(memory_space=pltpu.HBM),) * 2,
        scratch_shapes=[
            pltpu.VMEM(probes.shape, jnp.float32),
            pltpu.VMEM((count, cores * count), jnp.float32),
            pltpu.SemaphoreType.DMA((2, count + 1)),
        ],
        compiler_params=pltpu.CompilerParams(vmem_limit_bytes=60 * 1024 * 1024),
        name="hand_over",
    )(solved, summed)


def solution(mesh):
    in_specs = (
        P(("chain", "pa"), "gz", "gy", None),
        P(None, ("chain", "gz"), "gy", None),
        P(("chain", "gz"), "gy", None),
        P(("chain", "gz"), "gy", None),
        P(("chain", "gz"), "gy", None),
        P(("chain", "gz"), "gy", None),
    )
    out_specs = (P(("chain", "pa"), "gz", "gy", None), P(("chain", "pa"), None))
    return jax.shard_map(shards, mesh=mesh, in_specs=in_specs, out_specs=out_specs, check_vma=False)
```

```python
import functools

import jax
import jax.numpy as jnp
import numpy as np
from jax import lax
from jax.experimental import pallas as pl
from jax.experimental.pallas import tpu as pltpu
from jax.sharding import PartitionSpec as P

MESH = pl.DeviceIdType.MESH
STEPS = 5
SUB = 8

diffuse_cross = 0.15
diffuse_along = 16.0

ZLO, ZHI, YLO, YHI = range(4)
CZP, CZM, CYP, CYM, CXP, CXM, SRC, OBS = range(8)


def implicit_matrix(length):
    banded = (1.0 + 2.0 * diffuse_along) * np.eye(length) - diffuse_along * (
        np.eye(length, k=1) + np.eye(length, k=-1)
    )
    matrix = np.linalg.inv(banded).astype(np.float32)
    high = matrix.astype(jnp.bfloat16)
    low = (matrix - high.astype(np.float32)).astype(jnp.bfloat16)
    return jnp.asarray(high), jnp.asarray(low)


def kernel(
    *refs,
):
    inputs, (hessian_ref, gram_ref), refs = refs[:8], refs[8:10], refs[10:]
    loaded, refs = refs[:8], refs[8:]
    probes_ref, vel_ref, prior_ref, noise_ref, smask_ref, omask_ref, mhi_ref, mlo_ref = loaded
    (
    u_ref,
    s_ref,
    b_ref,
    coef_ref,
    whi_ref,
    wlo_ref,
    zh_ref,
    yh_ref,
    zs_ref,
    ys_ref,
    send_sem,
    recv_sem,
    load_sem,
    out_ref,
    out_sem,
    pu_ref,
    acc_ref,
    sum_ref,
    gt_ref,
    gr_ref,
    pair_send,
    pair_recv,
    ys_sem,
    yr_sem,
    zs_sem,
    zr_sem,
    core_sem,
    word_sem,
    ytile_ref,
    ztile_ref,
    ) = refs
    count, nz, ny, nx = probes_ref.shape
    tiles = ny // SUB
    zi, yi = lax.axis_index("gz"), lax.axis_index("gy")
    zn, yn = lax.axis_size("gz"), lax.axis_size("gy")
    exists = [zi > 0, zi < zn - 1, yi > 0, yi < yn - 1]
    target = [
        {"gz": lax.max(zi - 1, 0)},
        {"gz": lax.min(zi + 1, zn - 1)},
        {"gy": lax.max(yi - 1, 0)},
        {"gy": lax.min(yi + 1, yn - 1)},
    ]

    own = lax.axis_index("pa")
    half = nz // 2

    def crossed(me, distance):
        return me + distance * (1 - 2 * ((me // distance) % 2))

    def doubled(axis, me, n):
        return [{axis: crossed(me, 1 << k)} for k in range((n - 1).bit_length())]

    other_core = {"pa": 1 - own}
    y_doubled, z_doubled = doubled("gy", yi, yn), doubled("gz", zi, zn)
    z_other = zi - 1 + 2 * (zi % 2)
    y_other = yi - 1 + 2 * (yi % 2)
    met = [
        ((z_other >= 0) & (z_other < zn), {"gz": lax.clamp(0, z_other, zn - 1)}),
        ((y_other >= 0) & (y_other < yn), {"gy": lax.clamp(0, y_other, yn - 1)}),
    ]

    probe_loads = [
        pltpu.make_async_copy(inputs[0].at[p], probes_ref.at[p], load_sem.at[8 + p]) for p in range(count)
    ]
    loads = [None] + [pltpu.make_async_copy(inputs[k], loaded[k], load_sem.at[k]) for k in range(1, 8)]
    for copy in (loads[2], loads[4], probe_loads[0], loads[6], loads[7], *probe_loads[1:]):
        copy.start()
    for copy in (loads[1], loads[3], loads[5]):
        copy.start()

    barrier = pltpu.get_barrier_semaphore()
    greeted = [other_core] + y_doubled + z_doubled[:3]
    for device in greeted:
        pl.semaphore_signal(barrier, inc=1, device_id=device, device_id_type=MESH)
    for there, device in met:

        @pl.when(there)
        def _():
            pl.semaphore_signal(barrier, inc=1, device_id=device, device_id_type=MESH)

    row = lax.broadcasted_iota(jnp.int32, (SUB, nx), 0)
    first_row, last_row = row == 0, row == SUB - 1
    lane = lax.broadcasted_iota(jnp.int32, (ny, nx), 1)

    def prepare(z, _):
        vx, vy, vz = (0.5 * vel_ref[c, z] for c in range(3))
        coef_ref[CZP, z] = diffuse_cross - vz
        coef_ref[CZM, z] = diffuse_cross + vz
        coef_ref[CYP, z] = diffuse_cross - vy
        coef_ref[CYM, z] = diffuse_cross + vy
        coef_ref[CXP, z] = jnp.where(lane == nx - 1, 0.0, -vx)
        coef_ref[CXM, z] = jnp.where(lane == 0, 0.0, vx)
        coef_ref[OBS, z] = omask_ref[z].astype(jnp.float32) * noise_ref[z]
        return 0

    @pl.when(zi == 0)
    def _():
        zh_ref[:, 0] = jnp.zeros(zh_ref.shape[:1] + zh_ref.shape[2:], jnp.float32)

    @pl.when(zi == zn - 1)
    def _():
        zh_ref[:, 1] = jnp.zeros(zh_ref.shape[:1] + zh_ref.shape[2:], jnp.float32)

    @pl.when(yi == 0)
    def _():
        yh_ref[:, 0] = jnp.zeros(yh_ref.shape[:1] + yh_ref.shape[2:], jnp.float32)

    @pl.when(yi == yn - 1)
    def _():
        yh_ref[:, 1] = jnp.zeros(yh_ref.shape[:1] + yh_ref.shape[2:], jnp.float32)

    loads[2].wait()
    loads[4].wait()
    coef_ref[SRC] = smask_ref[...].astype(jnp.float32) * prior_ref[...]
    loads[6].wait()
    loads[7].wait()
    pl.semaphore_wait(barrier, len(greeted) + sum(there.astype(jnp.int32) for there, _ in met))

    def copies(slot, q, sources):
        result = []
        for side in range(4):
            halo = zh_ref if side < 2 else yh_ref
            result.append(
                pltpu.make_async_remote_copy(
                    src_ref=sources[side],
                    dst_ref=halo.at[slot, (side % 2) ^ 1, pl.ds(2 * q, 2)],
                    send_sem=send_sem.at[slot, side, q],
                    recv_sem=recv_sem.at[slot, side ^ 1, q],
                    device_id=target[side],
                    device_id_type=MESH,
                )
            )
        return result

    def send(slot, q, sources):
        for side, copy in enumerate(copies(slot, q, sources)):
            pl.when(exists[side])(copy.start)

    def settle(slot, q, sources):
        moved = copies(slot, q, sources)
        for side in range(4):

            @pl.when(exists[side])
            def _():
                moved[side ^ 1].wait_recv()
                moved[side].wait_send()

    def state_sources(n, slot, q):
        two = pl.ds(2 * q, 2)
        return [u_ref.at[n, two, 0], u_ref.at[n, two, nz - 1], ys_ref.at[slot, 0, two], ys_ref.at[slot, 1, two]]

    def adjoint_sources(slot, q):
        return [source.at[slot, side, pl.ds(2 * q, 2)] for source in (zs_ref, ys_ref) for side in range(2)]

    def both(q, *parts):
        for part in parts:
            for r in range(2):
                part(r, 2 * q + r)

    def put(r, z, pair, left, right):
        rows = jnp.concatenate([left, right], axis=0)
        high = rows.astype(jnp.bfloat16)
        low = (rows - high.astype(jnp.float32)).astype(jnp.bfloat16)
        where = pl.ds(z * ny + pair * 2 * SUB, 2 * SUB)
        whi_ref[r, where, :] = high
        wlo_ref[r, where, :] = low

    def solve(r):
        dot = functools.partial(jnp.dot, preferred_element_type=jnp.float32)
        high, low = whi_ref[r], wlo_ref[r]
        moved = dot(high, mhi_ref[...]) + (dot(high, mlo_ref[...]) + dot(low, mhi_ref[...]))
        return moved.reshape(nz, ny, nx)

    def by_tile(r, make):
        for z in range(nz):
            for pair in range(tiles // 2):
                put(r, z, pair, make(z, 2 * pair), make(z, 2 * pair + 1))

    def rows_of(t):
        return pl.ds(t * SUB, SUB)

    def coef(kind, z, t):
        return coef_ref[kind, z, rows_of(t), :]

    def forward(r, n, slot, p):
        def make(z, t):
            def at(zz, tt):
                return u_ref[n, p, zz, rows_of(tt), :]

            centre = at(z, t)
            plus_z = at(z + 1, t) if z < nz - 1 else zh_ref[slot, 1, p, rows_of(t), :]
            minus_z = at(z - 1, t) if z > 0 else zh_ref[slot, 0, p, rows_of(t), :]
            if t < tiles - 1:
                above = pltpu.roll(at(z, t + 1), SUB - 1, 0)
            else:
                above = jnp.broadcast_to(yh_ref[slot, 1, p, pl.ds(z, 1), :], (SUB, nx))
            if t > 0:
                below = pltpu.roll(at(z, t - 1), 1, 0)
            else:
                below = jnp.broadcast_to(yh_ref[slot, 0, p, pl.ds(z, 1), :], (SUB, nx))
            plus_y = jnp.where(last_row, above, pltpu.roll(centre, SUB - 1, 0))
            minus_y = jnp.where(first_row, below, pltpu.roll(centre, 1, 0))
            total = (1.0 - 4.0 * diffuse_cross) * centre + s_ref[p, z, rows_of(t), :]
            total = total + (coef(CZP, z, t) * plus_z + coef(CZM, z, t) * minus_z)
            total = total + (coef(CYP, z, t) * plus_y + coef(CYM, z, t) * minus_y)
            return total + (
                coef(CXP, z, t) * pltpu.roll(centre, nx - 1, 1) + coef(CXM, z, t) * pltpu.roll(centre, 1, 1)
            )

        by_tile(r, make)

    def backward(r, n, slot, p):
        def make(z, t):
            def at(zz, tt):
                return b_ref[p, zz, rows_of(tt), :]

            centre = at(z, t)
            if z < nz - 1:
                plus_z = coef(CZM, z + 1, t) * at(z + 1, t)
            else:
                plus_z = zh_ref[slot, 1, p, rows_of(t), :]
            if z > 0:
                minus_z = coef(CZP, z - 1, t) * at(z - 1, t)
            else:
                minus_z = zh_ref[slot, 0, p, rows_of(t), :]
            if t < tiles - 1:
                above = pltpu.roll(coef(CYM, z, t + 1) * at(z, t + 1), SUB - 1, 0)
            else:
                above = jnp.broadcast_to(yh_ref[slot, 1, p, pl.ds(z, 1), :], (SUB, nx))
            if t > 0:
                below = pltpu.roll(coef(CYP, z, t - 1) * at(z, t - 1), 1, 0)
            else:
                below = jnp.broadcast_to(yh_ref[slot, 0, p, pl.ds(z, 1), :], (SUB, nx))
            plus_y = jnp.where(last_row, above, pltpu.roll(coef(CYM, z, t) * centre, SUB - 1, 0))
            minus_y = jnp.where(first_row, below, pltpu.roll(coef(CYP, z, t) * centre, 1, 0))
            total = (1.0 - 4.0 * diffuse_cross) * centre + coef(OBS, z, t) * u_ref[n, p, z, rows_of(t), :]
            total = total + (plus_z + minus_z)
            total = total + (plus_y + minus_y)
            return total + (
                pltpu.roll(coef(CXM, z, t) * centre, nx - 1, 1) + pltpu.roll(coef(CXP, z, t) * centre, 1, 1)
            )

        by_tile(r, make)

    def finish_state(r, n, slot, p):
        state = solve(r)
        u_ref[n, p] = state
        for z in range(nz):
            ys_ref[slot, 0, p, pl.ds(z, 1), :] = state[z, 0:1, :]
            ys_ref[slot, 1, p, pl.ds(z, 1), :] = state[z, ny - 1 : ny, :]

    def finish_adjoint(slot, p, pulled):
        b_ref[p] = pulled
        zs_ref[slot, 0, p] = coef_ref[CZM, 0] * pulled[0]
        zs_ref[slot, 1, p] = coef_ref[CZP, nz - 1] * pulled[nz - 1]
        for z in range(nz):
            ys_ref[slot, 0, p, pl.ds(z, 1), :] = coef_ref[CYM, z, 0:1, :] * pulled[z, 0:1, :]
            ys_ref[slot, 1, p, pl.ds(z, 1), :] = coef_ref[CYP, z, ny - 1 : ny, :] * pulled[z, ny - 1 : ny, :]

    def pair_copy(n):
        return pltpu.make_async_remote_copy(
            src_ref=u_ref.at[n, :, pl.ds((1 - own) * half, half)],
            dst_ref=pu_ref.at[n],
            send_sem=pair_send.at[n],
            recv_sem=pair_recv.at[n],
            device_id=other_core,
            device_id_type=MESH,
        )

    def core_tile():
        return pltpu.make_async_remote_copy(
            src_ref=gt_ref.at[0],
            dst_ref=gr_ref,
            send_sem=core_sem.at[0],
            recv_sem=core_sem.at[1],
            device_id=other_core,
            device_id_type=MESH,
        )

    def along(axis, me, n, tiles_ref, source, out_sem, in_sem):
        def move(distance):
            return pltpu.make_async_remote_copy(
                src_ref=source,
                dst_ref=tiles_ref.at[me],
                send_sem=out_sem.at[distance],
                recv_sem=in_sem.at[me],
                device_id={axis: (me + distance) % n},
                device_id_type=MESH,
            )

        def arrival(who):
            return pltpu.make_async_remote_copy(
                src_ref=source,
                dst_ref=tiles_ref.at[who],
                send_sem=out_sem.at[0],
                recv_sem=in_sem.at[who],
                device_id={axis: (me + 1) % n},
                device_id_type=MESH,
            )

        def start():
            def step(distance, _):
                move(distance).start()
                return 0

            lax.fori_loop(1, n, step, 0)

        def end():
            def step(distance, _):
                arrival((me + distance) % n).wait_recv()
                move(distance).wait_send()
                return 0

            lax.fori_loop(1, n, step, 0)
            tiles_ref[me] = source[...]
            total = tiles_ref[0]
            for who in range(1, n):
                total = total + tiles_ref[who]
            return total

        return start, end

    start_y, end_y = along("gy", yi, yn, ytile_ref, gt_ref.at[2], ys_sem, yr_sem)
    start_z, end_z = along("gz", zi, zn, ztile_ref, gt_ref.at[3], zs_sem, zr_sem)

    def pass_word(k):
        if 0 < k <= len(z_doubled[:3]):
            pl.semaphore_wait(word_sem.at[k - 1], 1)
        if k < len(z_doubled[:3]):
            pl.semaphore_signal(word_sem.at[k], inc=1, device_id=z_doubled[k], device_id_type=MESH)

    near = count // 2 + 1
    lanes = 128
    pieces = [(t, h) for t in range(tiles) for h in range(nx // lanes)]

    def gram_unit(n, i):
        if count != 8:
            raise NotImplementedError
        wait_pair = pl.when(i == 0)

        @wait_pair
        def _():
            pair_copy(n).wait()

        def own_terms(k, sums):
            sums = list(sums)
            for z in (2 * k, 2 * k + 1):
                for t, h in pieces:
                    where = (rows_of(t), pl.ds(h * lanes, lanes))
                    x = [u_ref[(n, (i + d) % count, z) + where] for d in range(near + 1)]
                    weight = coef_ref[(OBS, z) + where]
                    for r in range(2):
                        scaled = weight * x[r]
                        for d in range(near):
                            sums[r * near + d] = sums[r * near + d] + scaled * x[r + d]
            return tuple(sums)

        def pair_terms(k, sums):
            sums = list(sums)
            for z in (2 * k, 2 * k + 1):
                for t, h in pieces:
                    where = (rows_of(t), pl.ds(h * lanes, lanes))
                    weight = coef_ref[(OBS, own * half + z) + where]
                    scaled = [weight * u_ref[(n, i + r, own * half + z) + where] for r in range(2)]
                    for j in range(count):
                        y = pu_ref[(n, j, z) + where]
                        for r in range(2):
                            sums[r * count + j] = sums[r * count + j] + scaled[r] * y
            return tuple(sums)

        zero = jnp.zeros((SUB, lanes), jnp.float32)
        sums = lax.fori_loop(0, nz // 2, own_terms, (zero,) * (2 * near))
        for r in range(2):
            for d in range(near):
                acc_ref[i + r, d] += sums[r * near + d]
        sums = lax.fori_loop(0, half // 2, pair_terms, (zero,) * (2 * count))
        for r in range(2):
            for j in range(count):
                acc_ref[i + r, near + j] += sums[r * count + j]

    def gram_units(n, first, units):
        def unit(k, _):
            gram_unit(n, 2 * (first + k))
            return 0

        lax.fori_loop(0, units, unit, 0)

    def gram_tile():
        ones = jnp.ones((lanes, lanes), jnp.float32)
        kinds = near + count

        def by_lanes(i, _):
            partial = acc_ref[i].reshape(kinds * SUB, lanes)
            total = jnp.dot(
                partial, ones, precision=lax.Precision.HIGHEST, preferred_element_type=jnp.float32
            )
            sum_ref[i] = total.reshape(kinds, SUB, lanes)
            return 0

        lax.fori_loop(0, count, by_lanes, 0)
        at_row = lax.broadcasted_iota(jnp.int32, (SUB, lanes), 0)
        at_lane = lax.broadcasted_iota(jnp.int32, (SUB, lanes), 1)
        mine, theirs = at_lane - own * count, at_lane - (1 - own) * count
        tile = jnp.zeros((SUB, lanes), jnp.float32)
        sent = jnp.zeros((SUB, lanes), jnp.float32)
        for i in range(count):
            for k in range(kinds):
                value = sum_ref[i, k]
                for shift in (4, 2, 1):
                    value = value + pltpu.roll(value, shift, 0)
                if k < near:
                    j = (i + k) % count
                    here = (at_row == i) & (mine == j)
                    if 0 < k < near - 1:
                        here = here | ((at_row == j) & (mine == i))
                    tile = tile + jnp.where(here, value, 0.0)
                else:
                    j = k - near
                    tile = tile + jnp.where((at_row == i) & (theirs == j), value, 0.0)
                    sent = sent + jnp.where((at_row == j) & (mine == i), value, 0.0)
        gt_ref[0] = sent
        gt_ref[1] = tile

    def end_core():
        core_tile().wait()
        gt_ref[2] = gt_ref[1] + gr_ref[...]
        start_y()

    def end_rows():
        gt_ref[3] = end_y()
        start_z()

    def out_copy(p):
        return pltpu.make_async_copy(out_ref.at[p], hessian_ref.at[p], out_sem.at[p])

    last = STEPS - 1

    pairs = count // 2

    def first_step(q, _):
        def source(r, p):
            pltpu.make_async_copy(inputs[0].at[p], probes_ref.at[p], load_sem.at[8 + p]).wait()
            for z in range(nz):
                for t in range(tiles):
                    s_ref[p, z, rows_of(t), :] = coef(SRC, z, t) * probes_ref[p, z, rows_of(t), :]
            by_tile(r, lambda z, t: coef(SRC, z, t) * probes_ref[p, z, rows_of(t), :])

        both(q, source, lambda r, p: finish_state(r, 0, 0, p))
        send(0, q, state_sources(0, 0, q))
        return 0

    lax.fori_loop(0, pairs, first_step, 0)
    pair_copy(0).start()
    acc_ref[...] = jnp.zeros(acc_ref.shape, jnp.float32)
    for k in (1, 3, 5):
        loads[k].wait()
    lax.fori_loop(0, nz, prepare, 0)

    def forward_step(i, _):
        n, q = i // pairs + 1, i % pairs
        before, now = (n + 1) % 2, n % 2
        settle(before, q, state_sources(n - 1, before, q))
        both(
            q,
            lambda r, p: forward(r, n - 1, before, p),
            lambda r, p: finish_state(r, n, now, p),
        )
        send(now, q, state_sources(n, now, q))

        @pl.when(q == pairs - 1)
        def _():
            pair_copy(n).start()
            gram_units(n - 1, 0, pairs)

        return 0

    lax.fori_loop(0, (last - 1) * pairs, forward_step, 0)

    def turn_step(q, _):
        before, now = (last + 1) % 2, last % 2
        settle(before, q, state_sources(last - 1, before, q))

        def turn(r, p):
            u_ref[last, p] = solve(r)
            by_tile(r, lambda z, t: coef(OBS, z, t) * u_ref[last, p, z, rows_of(t), :])

        def pull(r, p):
            pulled = solve(r)
            out_ref[p] = pulled
            finish_adjoint(now, p, pulled)

        both(q, lambda r, p: forward(r, last - 1, before, p), turn, pull)
        send(now, q, adjoint_sources(now, q))
        return 0

    lax.fori_loop(0, pairs, turn_step, 0)
    pair_copy(last).start()
    pass_word(0)
    gram_units(last - 1, 0, pairs)

    def backward_step(i, _):
        k, q = i // pairs + 1, i % pairs
        before, now = (last + k + 1) % 2, (last + k) % 2
        settle(before, q, adjoint_sources(before, q))

        def pull(r, p):
            pulled = solve(r)
            out_ref[p] += pulled
            finish_adjoint(now, p, pulled)

        both(q, lambda r, p: backward(r, last - k, before, p), pull)
        send(now, q, adjoint_sources(now, q))

        for turn, when in enumerate((0, 1, 3)):

            @pl.when(i == when)
            def _():
                pass_word(turn + 1)

        @pl.when(i < 2)
        def _():
            gram_units(last, 2 * i, 2)

        @pl.when(i == 1)
        def _():
            gram_tile()
            core_tile().start()

        pl.when(i == 2)(end_core)
        pl.when(i == 4)(end_rows)
        return 0

    lax.fori_loop(0, (last - 1) * pairs, backward_step, 0)

    def last_step(q, _):
        before = (2 * last + 1) % 2
        settle(before, q, adjoint_sources(before, q))

        def pull(r, p):
            out_ref[p] = coef_ref[SRC] * (out_ref[p] + solve(r))

        both(q, lambda r, p: backward(r, 0, before, p), pull, lambda r, p: out_copy(p).start())
        return 0

    lax.fori_loop(0, pairs, last_step, 0)
    for p in range(count):
        out_copy(p).wait()
    gram_ref[...] = end_z()[:, : gram_ref.shape[1]] / (nz * ny * nx * zn * yn)


def hand_over(solved_ref, summed_ref, hessian_ref, gram_ref, probe_ref, tile_ref, sem):
    count = solved_ref.shape[0]
    moves = [(solved_ref.at[p], probe_ref.at[p], hessian_ref.at[p]) for p in range(count)]
    moves.append((summed_ref, tile_ref, gram_ref))
    takes = [pltpu.make_async_copy(a, b, sem.at[0, k]) for k, (a, b, _) in enumerate(moves)]
    gives = [pltpu.make_async_copy(b, c, sem.at[1, k]) for k, (_, b, c) in enumerate(moves)]
    for take in takes:
        take.start()
    for take, give in zip(takes, gives):
        take.wait()
        give.start()
    for give in gives:
        give.wait()


def shards(probes, velocity, prior_scale, noise_precision, source_mask, sensor_mask):
    count, nz, ny, nx = probes.shape
    high, low = implicit_matrix(nx)
    arguments = (probes, velocity, prior_scale, noise_precision, source_mask, sensor_mask, high, low)
    cores = lax.axis_size("pa")
    zn, yn = lax.axis_size("gz"), lax.axis_size("gy")
    near = count // 2 + 1
    solved, summed = pl.pallas_call(
        kernel,
        out_shape=(
            jax.ShapeDtypeStruct(probes.shape, jnp.float32),
            jax.ShapeDtypeStruct((count, cores * count), jnp.float32),
        ),
        in_specs=[pl.BlockSpec(memory_space=pltpu.HBM)] * len(arguments),
        out_specs=(pl.BlockSpec(memory_space=pltpu.HBM), pl.BlockSpec(memory_space=pltpu.VMEM)),
        scratch_shapes=[
            *(pltpu.VMEM(array.shape, array.dtype) for array in arguments),
            pltpu.VMEM((STEPS, count, nz, ny, nx), jnp.float32),
            pltpu.VMEM((count, nz, ny, nx), jnp.float32),
            pltpu.VMEM((count, nz, ny, nx), jnp.float32),
            pltpu.VMEM((8, nz, ny, nx), jnp.float32),
            pltpu.VMEM((2, nz * ny, nx), jnp.bfloat16),
            pltpu.VMEM((2, nz * ny, nx), jnp.bfloat16),
            pltpu.VMEM((2, 2, count, ny, nx), jnp.float32),
            pltpu.VMEM((2, 2, count, nz, nx), jnp.float32),
            pltpu.VMEM((2, 2, count, ny, nx), jnp.float32),
            pltpu.VMEM((2, 2, count, nz, nx), jnp.float32),
            pltpu.SemaphoreType.DMA((2, 4, count // 2)),
            pltpu.SemaphoreType.DMA((2, 4, count // 2)),
            pltpu.SemaphoreType.DMA((8 + count,)),
            pltpu.VMEM((count, nz, ny, nx), jnp.float32),
            pltpu.SemaphoreType.DMA((count,)),
            pltpu.VMEM((STEPS, count, nz // 2, ny, nx), jnp.float32),
            pltpu.VMEM((count, near + count, SUB, 128), jnp.float32),
            pltpu.VMEM((count, near + count, SUB, 128), jnp.float32),
            pltpu.VMEM((4, SUB, 128), jnp.float32),
            pltpu.VMEM((SUB, 128), jnp.float32),
            pltpu.SemaphoreType.DMA((STEPS,)),
            pltpu.SemaphoreType.DMA((STEPS,)),
            pltpu.SemaphoreType.DMA((yn,)),
            pltpu.SemaphoreType.DMA((yn,)),
            pltpu.SemaphoreType.DMA((zn,)),
            pltpu.SemaphoreType.DMA((zn,)),
            pltpu.SemaphoreType.DMA((2,)),
            pltpu.SemaphoreType.REGULAR((3,)),
            pltpu.VMEM((yn, SUB, 128), jnp.float32),
            pltpu.VMEM((zn, SUB, 128), jnp.float32),
        ],
        compiler_params=pltpu.CompilerParams(
            collective_id=0, has_side_effects=True, vmem_limit_bytes=60 * 1024 * 1024
        ),
        name="solve",
    )(*arguments)
    return pl.pallas_call(
        hand_over,
        out_shape=(
            jax.ShapeDtypeStruct(probes.shape, jnp.float32),
            jax.ShapeDtypeStruct((count, cores * count), jnp.float32),
        ),
        in_specs=[pl.BlockSpec(memory_space=pltpu.HBM)] * 2,
        out_specs=(pl.BlockSpec(memory_space=pltpu.HBM),) * 2,
        scratch_shapes=[
            pltpu.VMEM(probes.shape, jnp.float32),
            pltpu.VMEM((count, cores * count), jnp.float32),
            pltpu.SemaphoreType.DMA((2, count + 1)),
        ],
        compiler_params=pltpu.CompilerParams(vmem_limit_bytes=60 * 1024 * 1024),
        name="hand_over",
    )(solved, summed)


def solution(mesh):
    in_specs = (
        P(("chain", "pa"), "gz", "gy", None),
        P(None, ("chain", "gz"), "gy", None),
        P(("chain", "gz"), "gy", None),
        P(("chain", "gz"), "gy", None),
        P(("chain", "gz"), "gy", None),
        P(("chain", "gz"), "gy", None),
    )
    out_specs = (P(("chain", "pa"), "gz", "gy", None), P(("chain", "pa"), None))
    return jax.shard_map(shards, mesh=mesh, in_specs=in_specs, out_specs=out_specs, check_vma=False)
```

```python
import functools

import jax
import jax.numpy as jnp
import numpy as np
from jax import lax
from jax.experimental import pallas as pl
from jax.experimental.pallas import tpu as pltpu
from jax.sharding import PartitionSpec as P

MESH = pl.DeviceIdType.MESH
STEPS = 5
SUB = 8

diffuse_cross = 0.15
diffuse_along = 16.0

ZLO, ZHI, YLO, YHI = range(4)
CZP, CZM, CYP, CYM, CXP, CXM, SRC, OBS = range(8)


def implicit_matrix(length):
    banded = (1.0 + 2.0 * diffuse_along) * np.eye(length) - diffuse_along * (
        np.eye(length, k=1) + np.eye(length, k=-1)
    )
    matrix = np.linalg.inv(banded).astype(np.float32)
    high = matrix.astype(jnp.bfloat16)
    low = (matrix - high.astype(np.float32)).astype(jnp.bfloat16)
    return jnp.asarray(high), jnp.asarray(low)


def kernel(
    *refs,
):
    inputs, (hessian_ref, gram_ref), refs = refs[:8], refs[8:10], refs[10:]
    loaded, refs = refs[:8], refs[8:]
    probes_ref, vel_ref, prior_ref, noise_ref, smask_ref, omask_ref, mhi_ref, mlo_ref = loaded
    (
    u_ref,
    s_ref,
    b_ref,
    coef_ref,
    whi_ref,
    wlo_ref,
    zh_ref,
    yh_ref,
    zs_ref,
    ys_ref,
    send_sem,
    recv_sem,
    load_sem,
    out_ref,
    out_sem,
    pu_ref,
    acc_ref,
    sum_ref,
    gt_ref,
    gr_ref,
    pair_send,
    pair_recv,
    ys_sem,
    yr_sem,
    zs_sem,
    zr_sem,
    core_sem,
    word_sem,
    ytile_ref,
    ztile_ref,
    ) = refs
    count, nz, ny, nx = probes_ref.shape
    tiles = ny // SUB
    zi, yi = lax.axis_index("gz"), lax.axis_index("gy")
    zn, yn = lax.axis_size("gz"), lax.axis_size("gy")
    exists = [zi > 0, zi < zn - 1, yi > 0, yi < yn - 1]
    target = [
        {"gz": lax.max(zi - 1, 0)},
        {"gz": lax.min(zi + 1, zn - 1)},
        {"gy": lax.max(yi - 1, 0)},
        {"gy": lax.min(yi + 1, yn - 1)},
    ]

    own = lax.axis_index("pa")
    half = nz // 2

    def crossed(me, distance):
        return me + distance * (1 - 2 * ((me // distance) % 2))

    def doubled(axis, me, n):
        return [{axis: crossed(me, 1 << k)} for k in range((n - 1).bit_length())]

    other_core = {"pa": 1 - own}
    y_doubled, z_doubled = doubled("gy", yi, yn), doubled("gz", zi, zn)
    z_other = zi - 1 + 2 * (zi % 2)
    y_other = yi - 1 + 2 * (yi % 2)
    met = [
        ((z_other >= 0) & (z_other < zn), {"gz": lax.clamp(0, z_other, zn - 1)}),
        ((y_other >= 0) & (y_other < yn), {"gy": lax.clamp(0, y_other, yn - 1)}),
    ]

    probe_loads = [
        pltpu.make_async_copy(inputs[0].at[p], probes_ref.at[p], load_sem.at[8 + p]) for p in range(count)
    ]
    loads = [None] + [pltpu.make_async_copy(inputs[k], loaded[k], load_sem.at[k]) for k in range(1, 8)]
    for copy in (loads[2], loads[4], probe_loads[0], loads[6], loads[7], *probe_loads[1:]):
        copy.start()
    for copy in (loads[1], loads[3], loads[5]):
        copy.start()

    barrier = pltpu.get_barrier_semaphore()
    greeted = [other_core] + y_doubled + z_doubled[:3]
    for device in greeted:
        pl.semaphore_signal(barrier, inc=1, device_id=device, device_id_type=MESH)
    for there, device in met:

        @pl.when(there)
        def _():
            pl.semaphore_signal(barrier, inc=1, device_id=device, device_id_type=MESH)

    row = lax.broadcasted_iota(jnp.int32, (SUB, nx), 0)
    first_row, last_row = row == 0, row == SUB - 1
    lane = lax.broadcasted_iota(jnp.int32, (ny, nx), 1)

    def prepare(z, _):
        vx, vy, vz = (0.5 * vel_ref[c, z] for c in range(3))
        coef_ref[CZP, z] = diffuse_cross - vz
        coef_ref[CZM, z] = diffuse_cross + vz
        coef_ref[CYP, z] = diffuse_cross - vy
        coef_ref[CYM, z] = diffuse_cross + vy
        coef_ref[CXP, z] = jnp.where(lane == nx - 1, 0.0, -vx)
        coef_ref[CXM, z] = jnp.where(lane == 0, 0.0, vx)
        coef_ref[OBS, z] = omask_ref[z].astype(jnp.float32) * noise_ref[z]
        return 0

    @pl.when(zi == 0)
    def _():
        zh_ref[:, 0] = jnp.zeros(zh_ref.shape[:1] + zh_ref.shape[2:], jnp.float32)

    @pl.when(zi == zn - 1)
    def _():
        zh_ref[:, 1] = jnp.zeros(zh_ref.shape[:1] + zh_ref.shape[2:], jnp.float32)

    @pl.when(yi == 0)
    def _():
        yh_ref[:, 0] = jnp.zeros(yh_ref.shape[:1] + yh_ref.shape[2:], jnp.float32)

    @pl.when(yi == yn - 1)
    def _():
        yh_ref[:, 1] = jnp.zeros(yh_ref.shape[:1] + yh_ref.shape[2:], jnp.float32)

    loads[2].wait()
    loads[4].wait()
    coef_ref[SRC] = smask_ref[...].astype(jnp.float32) * prior_ref[...]
    loads[6].wait()
    loads[7].wait()
    pl.semaphore_wait(barrier, len(greeted) + sum(there.astype(jnp.int32) for there, _ in met))

    def copies(slot, q, sources):
        result = []
        for side in range(4):
            halo = zh_ref if side < 2 else yh_ref
            result.append(
                pltpu.make_async_remote_copy(
                    src_ref=sources[side],
                    dst_ref=halo.at[slot, (side % 2) ^ 1, pl.ds(2 * q, 2)],
                    send_sem=send_sem.at[slot, side, q],
                    recv_sem=recv_sem.at[slot, side ^ 1, q],
                    device_id=target[side],
                    device_id_type=MESH,
                )
            )
        return result

    def send(slot, q, sources):
        for side, copy in enumerate(copies(slot, q, sources)):
            pl.when(exists[side])(copy.start)

    def settle(slot, q, sources):
        moved = copies(slot, q, sources)
        for side in range(4):

            @pl.when(exists[side])
            def _():
                moved[side ^ 1].wait_recv()
                moved[side].wait_send()

    def state_sources(n, slot, q):
        two = pl.ds(2 * q, 2)
        return [u_ref.at[n, two, 0], u_ref.at[n, two, nz - 1], ys_ref.at[slot, 0, two], ys_ref.at[slot, 1, two]]

    def adjoint_sources(slot, q):
        return [source.at[slot, side, pl.ds(2 * q, 2)] for source in (zs_ref, ys_ref) for side in range(2)]

    def both(q, *parts):
        for part in parts:
            for r in range(2):
                part(r, 2 * q + r)

    def put(r, z, pair, left, right):
        rows = jnp.concatenate([left, right], axis=0)
        high = rows.astype(jnp.bfloat16)
        low = (rows - high.astype(jnp.float32)).astype(jnp.bfloat16)
        where = pl.ds(z * ny + pair * 2 * SUB, 2 * SUB)
        whi_ref[r, where, :] = high
        wlo_ref[r, where, :] = low

    def solve(r):
        dot = functools.partial(jnp.dot, preferred_element_type=jnp.float32)
        high, low = whi_ref[r], wlo_ref[r]
        moved = dot(high, mhi_ref[...]) + (dot(high, mlo_ref[...]) + dot(low, mhi_ref[...]))
        return moved.reshape(nz, ny, nx)

    def by_tile(r, make):
        for z in range(nz):
            for pair in range(tiles // 2):
                put(r, z, pair, make(z, 2 * pair), make(z, 2 * pair + 1))

    def rows_of(t):
        return pl.ds(t * SUB, SUB)

    def coef(kind, z, t):
        return coef_ref[kind, z, rows_of(t), :]

    def forward(r, n, slot, p):
        def make(z, t):
            def at(zz, tt):
                return u_ref[n, p, zz, rows_of(tt), :]

            centre = at(z, t)
            plus_z = at(z + 1, t) if z < nz - 1 else zh_ref[slot, 1, p, rows_of(t), :]
            minus_z = at(z - 1, t) if z > 0 else zh_ref[slot, 0, p, rows_of(t), :]
            if t < tiles - 1:
                above = pltpu.roll(at(z, t + 1), SUB - 1, 0)
            else:
                above = jnp.broadcast_to(yh_ref[slot, 1, p, pl.ds(z, 1), :], (SUB, nx))
            if t > 0:
                below = pltpu.roll(at(z, t - 1), 1, 0)
            else:
                below = jnp.broadcast_to(yh_ref[slot, 0, p, pl.ds(z, 1), :], (SUB, nx))
            plus_y = jnp.where(last_row, above, pltpu.roll(centre, SUB - 1, 0))
            minus_y = jnp.where(first_row, below, pltpu.roll(centre, 1, 0))
            total = (1.0 - 4.0 * diffuse_cross) * centre + s_ref[p, z, rows_of(t), :]
            total = total + (coef(CZP, z, t) * plus_z + coef(CZM, z, t) * minus_z)
            total = total + (coef(CYP, z, t) * plus_y + coef(CYM, z, t) * minus_y)
            return total + (
                coef(CXP, z, t) * pltpu.roll(centre, nx - 1, 1) + coef(CXM, z, t) * pltpu.roll(centre, 1, 1)
            )

        by_tile(r, make)

    def backward(r, n, slot, p):
        def make(z, t):
            def at(zz, tt):
                return b_ref[p, zz, rows_of(tt), :]

            centre = at(z, t)
            if z < nz - 1:
                plus_z = coef(CZM, z + 1, t) * at(z + 1, t)
            else:
                plus_z = zh_ref[slot, 1, p, rows_of(t), :]
            if z > 0:
                minus_z = coef(CZP, z - 1, t) * at(z - 1, t)
            else:
                minus_z = zh_ref[slot, 0, p, rows_of(t), :]
            if t < tiles - 1:
                above = pltpu.roll(coef(CYM, z, t + 1) * at(z, t + 1), SUB - 1, 0)
            else:
                above = jnp.broadcast_to(yh_ref[slot, 1, p, pl.ds(z, 1), :], (SUB, nx))
            if t > 0:
                below = pltpu.roll(coef(CYP, z, t - 1) * at(z, t - 1), 1, 0)
            else:
                below = jnp.broadcast_to(yh_ref[slot, 0, p, pl.ds(z, 1), :], (SUB, nx))
            plus_y = jnp.where(last_row, above, pltpu.roll(coef(CYM, z, t) * centre, SUB - 1, 0))
            minus_y = jnp.where(first_row, below, pltpu.roll(coef(CYP, z, t) * centre, 1, 0))
            total = (1.0 - 4.0 * diffuse_cross) * centre + coef(OBS, z, t) * u_ref[n, p, z, rows_of(t), :]
            total = total + (plus_z + minus_z)
            total = total + (plus_y + minus_y)
            return total + (
                pltpu.roll(coef(CXM, z, t) * centre, nx - 1, 1) + pltpu.roll(coef(CXP, z, t) * centre, 1, 1)
            )

        by_tile(r, make)

    def finish_state(r, n, slot, p):
        state = solve(r)
        u_ref[n, p] = state
        for z in range(nz):
            ys_ref[slot, 0, p, pl.ds(z, 1), :] = state[z, 0:1, :]
            ys_ref[slot, 1, p, pl.ds(z, 1), :] = state[z, ny - 1 : ny, :]

    def finish_adjoint(slot, p, pulled):
        b_ref[p] = pulled
        zs_ref[slot, 0, p] = coef_ref[CZM, 0] * pulled[0]
        zs_ref[slot, 1, p] = coef_ref[CZP, nz - 1] * pulled[nz - 1]
        for z in range(nz):
            ys_ref[slot, 0, p, pl.ds(z, 1), :] = coef_ref[CYM, z, 0:1, :] * pulled[z, 0:1, :]
            ys_ref[slot, 1, p, pl.ds(z, 1), :] = coef_ref[CYP, z, ny - 1 : ny, :] * pulled[z, ny - 1 : ny, :]

    def pair_copy(n):
        return pltpu.make_async_remote_copy(
            src_ref=u_ref.at[n, :, pl.ds((1 - own) * half, half)],
            dst_ref=pu_ref.at[n],
            send_sem=pair_send.at[n],
            recv_sem=pair_recv.at[n],
            device_id=other_core,
            device_id_type=MESH,
        )

    def core_tile():
        return pltpu.make_async_remote_copy(
            src_ref=gt_ref.at[0],
            dst_ref=gr_ref,
            send_sem=core_sem.at[0],
            recv_sem=core_sem.at[1],
            device_id=other_core,
            device_id_type=MESH,
        )

    def along(axis, me, n, tiles_ref, source, out_sem, in_sem):
        def move(distance):
            return pltpu.make_async_remote_copy(
                src_ref=source,
                dst_ref=tiles_ref.at[me],
                send_sem=out_sem.at[distance],
                recv_sem=in_sem.at[me],
                device_id={axis: (me + distance) % n},
                device_id_type=MESH,
            )

        def arrival(who):
            return pltpu.make_async_remote_copy(
                src_ref=source,
                dst_ref=tiles_ref.at[who],
                send_sem=out_sem.at[0],
                recv_sem=in_sem.at[who],
                device_id={axis: (me + 1) % n},
                device_id_type=MESH,
            )

        def start():
            def step(distance, _):
                move(distance).start()
                return 0

            lax.fori_loop(1, n, step, 0)

        def end():
            def step(distance, _):
                arrival((me + distance) % n).wait_recv()
                move(distance).wait_send()
                return 0

            lax.fori_loop(1, n, step, 0)
            tiles_ref[me] = source[...]
            total = tiles_ref[0]
            for who in range(1, n):
                total = total + tiles_ref[who]
            return total

        return start, end

    start_y, end_y = along("gy", yi, yn, ytile_ref, gt_ref.at[2], ys_sem, yr_sem)
    start_z, end_z = along("gz", zi, zn, ztile_ref, gt_ref.at[3], zs_sem, zr_sem)

    def pass_word(k):
        if 0 < k <= len(z_doubled[:3]):
            pl.semaphore_wait(word_sem.at[k - 1], 1)
        if k < len(z_doubled[:3]):
            pl.semaphore_signal(word_sem.at[k], inc=1, device_id=z_doubled[k], device_id_type=MESH)

    near = count // 2 + 1
    lanes = 128
    pieces = [(t, h) for t in range(tiles) for h in range(nx // lanes)]

    def gram_unit(n, i):
        if count != 8:
            raise NotImplementedError
        wait_pair = pl.when(i == 0)

        @wait_pair
        def _():
            pair_copy(n).wait()

        def own_terms(k, sums):
            sums = list(sums)
            for z in (2 * k, 2 * k + 1):
                for t, h in pieces:
                    where = (rows_of(t), pl.ds(h * lanes, lanes))
                    x = [u_ref[(n, (i + d) % count, z) + where] for d in range(near + 1)]
                    weight = coef_ref[(OBS, z) + where]
                    for r in range(2):
                        scaled = weight * x[r]
                        for d in range(near):
                            sums[r * near + d] = sums[r * near + d] + scaled * x[r + d]
            return tuple(sums)

        def pair_terms(k, sums):
            sums = list(sums)
            for z in (2 * k, 2 * k + 1):
                for t, h in pieces:
                    where = (rows_of(t), pl.ds(h * lanes, lanes))
                    weight = coef_ref[(OBS, own * half + z) + where]
                    scaled = [weight * u_ref[(n, i + r, own * half + z) + where] for r in range(2)]
                    for j in range(count):
                        y = pu_ref[(n, j, z) + where]
                        for r in range(2):
                            sums[r * count + j] = sums[r * count + j] + scaled[r] * y
            return tuple(sums)

        zero = jnp.zeros((SUB, lanes), jnp.float32)
        sums = lax.fori_loop(0, nz // 2, own_terms, (zero,) * (2 * near))
        for r in range(2):
            for d in range(near):
                acc_ref[i + r, d] += sums[r * near + d]
        sums = lax.fori_loop(0, half // 2, pair_terms, (zero,) * (2 * count))
        for r in range(2):
            for j in range(count):
                acc_ref[i + r, near + j] += sums[r * count + j]

    def gram_units(n, first, units):
        def unit(k, _):
            gram_unit(n, 2 * (first + k))
            return 0

        lax.fori_loop(0, units, unit, 0)

    def gram_tile():
        ones = jnp.ones((lanes, lanes), jnp.float32)
        kinds = near + count

        def by_lanes(i, _):
            partial = acc_ref[i].reshape(kinds * SUB, lanes)
            total = jnp.dot(
                partial, ones, precision=lax.Precision.HIGHEST, preferred_element_type=jnp.float32
            )
            sum_ref[i] = total.reshape(kinds, SUB, lanes)
            return 0

        lax.fori_loop(0, count, by_lanes, 0)
        at_row = lax.broadcasted_iota(jnp.int32, (SUB, lanes), 0)
        at_lane = lax.broadcasted_iota(jnp.int32, (SUB, lanes), 1)
        mine, theirs = at_lane - own * count, at_lane - (1 - own) * count
        tile = jnp.zeros((SUB, lanes), jnp.float32)
        sent = jnp.zeros((SUB, lanes), jnp.float32)
        for i in range(count):
            for k in range(kinds):
                value = sum_ref[i, k]
                for shift in (4, 2, 1):
                    value = value + pltpu.roll(value, shift, 0)
                if k < near:
                    j = (i + k) % count
                    here = (at_row == i) & (mine == j)
                    if 0 < k < near - 1:
                        here = here | ((at_row == j) & (mine == i))
                    tile = tile + jnp.where(here, value, 0.0)
                else:
                    j = k - near
                    tile = tile + jnp.where((at_row == i) & (theirs == j), value, 0.0)
                    sent = sent + jnp.where((at_row == j) & (mine == i), value, 0.0)
        gt_ref[0] = sent
        gt_ref[1] = tile

    def end_core():
        core_tile().wait()
        gt_ref[2] = gt_ref[1] + gr_ref[...]
        start_y()

    def end_rows():
        gt_ref[3] = end_y()
        start_z()

    def out_copy(p):
        return pltpu.make_async_copy(out_ref.at[p], hessian_ref.at[p], out_sem.at[p])

    last = STEPS - 1

    pairs = count // 2

    def first_step(q, _):
        def source(r, p):
            pltpu.make_async_copy(inputs[0].at[p], probes_ref.at[p], load_sem.at[8 + p]).wait()
            for z in range(nz):
                for t in range(tiles):
                    s_ref[p, z, rows_of(t), :] = coef(SRC, z, t) * probes_ref[p, z, rows_of(t), :]
            by_tile(r, lambda z, t: coef(SRC, z, t) * probes_ref[p, z, rows_of(t), :])

        both(q, source, lambda r, p: finish_state(r, 0, 0, p))
        send(0, q, state_sources(0, 0, q))
        return 0

    lax.fori_loop(0, pairs, first_step, 0)
    pair_copy(0).start()
    acc_ref[...] = jnp.zeros(acc_ref.shape, jnp.float32)
    for k in (1, 3, 5):
        loads[k].wait()
    lax.fori_loop(0, nz, prepare, 0)

    def forward_step(i, _):
        n, q = i // pairs + 1, i % pairs
        before, now = (n + 1) % 2, n % 2
        settle(before, q, state_sources(n - 1, before, q))
        both(
            q,
            lambda r, p: forward(r, n - 1, before, p),
            lambda r, p: finish_state(r, n, now, p),
        )
        send(now, q, state_sources(n, now, q))

        @pl.when(q == pairs - 1)
        def _():
            pair_copy(n).start()
            gram_units(n - 1, 0, pairs)

        return 0

    lax.fori_loop(0, (last - 1) * pairs, forward_step, 0)

    def turn_step(q, _):
        before, now = (last + 1) % 2, last % 2
        settle(before, q, state_sources(last - 1, before, q))

        def turn(r, p):
            u_ref[last, p] = solve(r)
            by_tile(r, lambda z, t: coef(OBS, z, t) * u_ref[last, p, z, rows_of(t), :])

        def pull(r, p):
            pulled = solve(r)
            out_ref[p] = pulled
            finish_adjoint(now, p, pulled)

        both(q, lambda r, p: forward(r, last - 1, before, p), turn, pull)
        send(now, q, adjoint_sources(now, q))
        return 0

    lax.fori_loop(0, pairs, turn_step, 0)
    pair_copy(last).start()
    pass_word(0)

    def backward_step(i, _):
        k, q = i // pairs + 1, i % pairs
        before, now = (last + k + 1) % 2, (last + k) % 2
        settle(before, q, adjoint_sources(before, q))

        def pull(r, p):
            pulled = solve(r)
            out_ref[p] += pulled
            finish_adjoint(now, p, pulled)

        both(q, lambda r, p: backward(r, last - k, before, p), pull)
        send(now, q, adjoint_sources(now, q))

        for turn, when in enumerate((0, 2, 4)):

            @pl.when(i == when)
            def _():
                pass_word(turn + 1)

        @pl.when(i < 4)
        def _():
            gram_units(last - 1 + i // 2, 2 * (i % 2), 2)

        @pl.when(i == 3)
        def _():
            gram_tile()
            core_tile().start()

        pl.when(i == 4)(end_core)
        pl.when(i == 5)(end_rows)
        return 0

    lax.fori_loop(0, (last - 1) * pairs, backward_step, 0)

    def last_step(q, _):
        before = (2 * last + 1) % 2
        settle(before, q, adjoint_sources(before, q))

        def pull(r, p):
            out_ref[p] = coef_ref[SRC] * (out_ref[p] + solve(r))

        both(q, lambda r, p: backward(r, 0, before, p), pull, lambda r, p: out_copy(p).start())
        return 0

    lax.fori_loop(0, pairs, last_step, 0)
    for p in range(count):
        out_copy(p).wait()
    gram_ref[...] = end_z()[:, : gram_ref.shape[1]] / (nz * ny * nx * zn * yn)


def hand_over(solved_ref, summed_ref, hessian_ref, gram_ref, probe_ref, tile_ref, sem):
    count = solved_ref.shape[0]
    moves = [(solved_ref.at[p], probe_ref.at[p], hessian_ref.at[p]) for p in range(count)]
    moves.append((summed_ref, tile_ref, gram_ref))
    takes = [pltpu.make_async_copy(a, b, sem.at[0, k]) for k, (a, b, _) in enumerate(moves)]
    gives = [pltpu.make_async_copy(b, c, sem.at[1, k]) for k, (_, b, c) in enumerate(moves)]
    for take in takes:
        take.start()
    for take, give in zip(takes, gives):
        take.wait()
        give.start()
    for give in gives:
        give.wait()


def shards(probes, velocity, prior_scale, noise_precision, source_mask, sensor_mask):
    count, nz, ny, nx = probes.shape
    high, low = implicit_matrix(nx)
    arguments = (probes, velocity, prior_scale, noise_precision, source_mask, sensor_mask, high, low)
    cores = lax.axis_size("pa")
    zn, yn = lax.axis_size("gz"), lax.axis_size("gy")
    near = count // 2 + 1
    solved, summed = pl.pallas_call(
        kernel,
        out_shape=(
            jax.ShapeDtypeStruct(probes.shape, jnp.float32),
            jax.ShapeDtypeStruct((count, cores * count), jnp.float32),
        ),
        in_specs=[pl.BlockSpec(memory_space=pltpu.HBM)] * len(arguments),
        out_specs=(pl.BlockSpec(memory_space=pltpu.HBM), pl.BlockSpec(memory_space=pltpu.VMEM)),
        scratch_shapes=[
            *(pltpu.VMEM(array.shape, array.dtype) for array in arguments),
            pltpu.VMEM((STEPS, count, nz, ny, nx), jnp.float32),
            pltpu.VMEM((count, nz, ny, nx), jnp.float32),
            pltpu.VMEM((count, nz, ny, nx), jnp.float32),
            pltpu.VMEM((8, nz, ny, nx), jnp.float32),
            pltpu.VMEM((2, nz * ny, nx), jnp.bfloat16),
            pltpu.VMEM((2, nz * ny, nx), jnp.bfloat16),
            pltpu.VMEM((2, 2, count, ny, nx), jnp.float32),
            pltpu.VMEM((2, 2, count, nz, nx), jnp.float32),
            pltpu.VMEM((2, 2, count, ny, nx), jnp.float32),
            pltpu.VMEM((2, 2, count, nz, nx), jnp.float32),
            pltpu.SemaphoreType.DMA((2, 4, count // 2)),
            pltpu.SemaphoreType.DMA((2, 4, count // 2)),
            pltpu.SemaphoreType.DMA((8 + count,)),
            pltpu.VMEM((count, nz, ny, nx), jnp.float32),
            pltpu.SemaphoreType.DMA((count,)),
            pltpu.VMEM((STEPS, count, nz // 2, ny, nx), jnp.float32),
            pltpu.VMEM((count, near + count, SUB, 128), jnp.float32),
            pltpu.VMEM((count, near + count, SUB, 128), jnp.float32),
            pltpu.VMEM((4, SUB, 128), jnp.float32),
            pltpu.VMEM((SUB, 128), jnp.float32),
            pltpu.SemaphoreType.DMA((STEPS,)),
            pltpu.SemaphoreType.DMA((STEPS,)),
            pltpu.SemaphoreType.DMA((yn,)),
            pltpu.SemaphoreType.DMA((yn,)),
            pltpu.SemaphoreType.DMA((zn,)),
            pltpu.SemaphoreType.DMA((zn,)),
            pltpu.SemaphoreType.DMA((2,)),
            pltpu.SemaphoreType.REGULAR((3,)),
            pltpu.VMEM((yn, SUB, 128), jnp.float32),
            pltpu.VMEM((zn, SUB, 128), jnp.float32),
        ],
        compiler_params=pltpu.CompilerParams(
            collective_id=0, has_side_effects=True, vmem_limit_bytes=60 * 1024 * 1024
        ),
        name="solve",
    )(*arguments)
    return pl.pallas_call(
        hand_over,
        out_shape=(
            jax.ShapeDtypeStruct(probes.shape, jnp.float32),
            jax.ShapeDtypeStruct((count, cores * count), jnp.float32),
        ),
        in_specs=[pl.BlockSpec(memory_space=pltpu.HBM)] * 2,
        out_specs=(pl.BlockSpec(memory_space=pltpu.HBM),) * 2,
        scratch_shapes=[
            pltpu.VMEM(probes.shape, jnp.float32),
            pltpu.VMEM((count, cores * count), jnp.float32),
            pltpu.SemaphoreType.DMA((2, count + 1)),
        ],
        compiler_params=pltpu.CompilerParams(vmem_limit_bytes=60 * 1024 * 1024),
        name="hand_over",
    )(solved, summed)


def solution(mesh):
    in_specs = (
        P(("chain", "pa"), "gz", "gy", None),
        P(None, ("chain", "gz"), "gy", None),
        P(("chain", "gz"), "gy", None),
        P(("chain", "gz"), "gy", None),
        P(("chain", "gz"), "gy", None),
        P(("chain", "gz"), "gy", None),
    )
    out_specs = (P(("chain", "pa"), "gz", "gy", None), P(("chain", "pa"), None))
    return jax.shard_map(shards, mesh=mesh, in_specs=in_specs, out_specs=out_specs, check_vma=False)
```
